32 devices in a mesh: wide: 16 (over z, y, x), narrow: 2 (over core).
Axes of the slice: x: 2, y: 2, z: 4, core: 2. Of those that a mesh axis runs over, the one named last changes fastest.
Arguments:
- electric: float32 [3, 3, 128, 48, 128], P(None, None, 'wide', 'narrow'), may hold values from -6 to 6
- magnetic: float32 [3, 3, 128, 48, 128], P(None, None, 'wide', 'narrow'), may hold values from -6 to 6
- current: float32 [3, 128, 48, 128], P(None, 'wide', 'narrow'), may hold values from -6 to 6
- density_tiles: float32 [64, 24, 64], P('wide', 'narrow'), may hold values from 0 to 1
- tile_slabs: int32 [16], replicated, may hold values from 0 to 15, each once
- design_box: int32 [6], replicated, may hold values from 0 to 128, as said below
- material_mask: int32 [128, 48, 128], P('wide', 'narrow'), may hold values 0 or 1
- material_levels: float32 [2], replicated, may hold values from 2 to 12
Outputs:
- final_electric: float32 [3, 3, 128, 48, 128], P(None, None, 'wide', 'narrow')
- final_magnetic: float32 [3, 3, 128, 48, 128], P(None, None, 'wide', 'narrow')
The draws below stay inside these ranges and needn't reach their ends.
Inputs may be any that keep to these rules, and one draw needn't show every extreme that they name: `tile_slabs`: each slab index appears exactly once. `design_box`: along each dimension of n cells the low bound is below n // 4; the high bound is 128 along the first dimension, at least 24 along the second, and at least n // 2 along the third.
All inputs are finite; a program needn't handle non-finite values. No bound on the sum of `material_mask` on one device may be relied on, other than what follows from the above.
Results may differ from the reference program's by a relative error of at most 0.00013.
Values sent between devices are 32-bit elements; how exact they have to be, the bound alone decides.
A program may use at most 64 MiB of HBM per device.

```python
import jax
import jax.numpy as jnp
from jax import lax

CX = 8
CY = 24
STEPS = 4
REALS = 3
NX = 128
NY = 48
NZ = 128
N_WIDE = 16


def draw_design_box(key, part):
    subkeys = jax.random.split(key, 6)
    x_low = jax.random.randint(subkeys[0], (1,), 0, NX // 4, dtype=jnp.int32)
    x_high = jnp.full((1,), NX, dtype=jnp.int32)
    y_low = jax.random.randint(subkeys[2], (1,), 0, NY // 4, dtype=jnp.int32)
    y_high = jax.random.randint(subkeys[3], (1,), NY - CY, NY + 1, dtype=jnp.int32)
    z_low = jax.random.randint(subkeys[4], (1,), 0, NZ // 4, dtype=jnp.int32)
    z_high = jax.random.randint(subkeys[5], (1,), NZ // 2, NZ + 1, dtype=jnp.int32)
    return jnp.concatenate([x_low, x_high, y_low, y_high, z_low, z_high]).astype(jnp.int32)


def place_ends(entries, stream_key, low, top_value):
    place = [jax.random.randint(jax.random.fold_in(stream_key, axis), (), 0, length) for axis, length in enumerate(entries.shape)]
    longest = entries.shape.index(max(entries.shape))
    next_to = place[:longest] + [(place[longest] + 1) % entries.shape[longest]] + place[longest + 1:]
    return entries.at[tuple(place)].set(low).at[tuple(next_to)].set(top_value)


def block_levels(rng, dims, cuts, smallest, top_value):
    def one(position, shards_of):
        heights = jax.random.uniform(jax.random.fold_in(jax.random.fold_in(rng, 6), position), (shards_of,), jnp.float32, smallest / len(cuts), top_value / len(cuts))
        return jnp.repeat(jnp.exp(heights), dims[position] // shards_of).reshape((-1,) + (1,) * (len(dims) - position - 1))

    factor_of = one(*cuts[0])
    for cut in cuts[1:]:
        factor_of = factor_of * one(*cut)
    return factor_of


def normal_values(key, dims, spread, most, cuts=(), kind=jnp.bfloat16):
    factor_of = block_levels(key, dims, cuts, -0.22, 0.18) if cuts else 1.0
    drawn = jax.random.normal(key, dims, jnp.float32) * spread * factor_of
    return jnp.minimum(jnp.maximum(drawn, -most), most).astype(kind)


def setup_inputs(seed: int = 0) -> dict:
    seeds = jax.random.split(jax.random.key(seed), 9)
    electric = normal_values(seeds[0], (REALS, 3, NX, NY, NZ), 1.0, 6.0, ((2, 16), (3, 2)), jnp.float32)
    magnetic = normal_values(seeds[1], (REALS, 3, NX, NY, NZ), 1.0, 6.0, ((2, 16), (3, 2)), jnp.float32)
    current = normal_values(seeds[2], (3, NX, NY, NZ), 1.0, 6.0, ((1, 16), (2, 2)), jnp.float32)
    density_tiles = jnp.clip(1.0 * jax.random.uniform(seeds[3], (NX // 2, NY // 2, NZ // 2), jnp.float32) ** block_levels(seeds[3], (NX // 2, NY // 2, NZ // 2), ((0, 16), (1, 2)), -0.2, 0.2), 0.0, 1.0)
    tile_slabs = jax.random.permutation(seeds[4], N_WIDE).astype(jnp.int32)
    design_box = draw_design_box(jax.random.fold_in(seeds[8], 71), 0)
    material_mask = place_ends((jax.random.randint(seeds[6], (NX, NY, NZ), 0, 2) < 1).astype(jnp.int32), jax.random.fold_in(seeds[6], 1), 0, 1)
    material_levels = jnp.clip(jax.random.uniform(seeds[7], (2,), jnp.float32, 2.0, 12.0), 2.0, 12.0)
    return dict(electric=electric, magnetic=magnetic, current=current, density_tiles=density_tiles, tile_slabs=tile_slabs, design_box=design_box, material_mask=material_mask, material_levels=material_levels)


sharpness = 8.0
thresholds = (0.7, 0.5, 0.3)
time_step = 0.5


def project(filtered, threshold):
    numer = jnp.tanh(sharpness * threshold) + jnp.tanh(sharpness * (filtered - threshold))
    denom = jnp.tanh(sharpness * threshold) + jnp.tanh(sharpness * (1.0 - threshold))
    return numer / denom


def refine(extended, dimension):
    cells_in = extended.shape[dimension] - 1
    lower_cells = lax.slice_in_dim(extended, 0, cells_in, axis=dimension)
    higher_cells = lax.slice_in_dim(extended, 1, cells_in + 1, axis=dimension)
    middle = 0.5 * (lower_cells + higher_cells)
    paired = jnp.stack([lower_cells, middle], axis=dimension + 1)
    new_shape = list(extended.shape)
    new_shape[dimension] = 2 * cells_in
    return paired.reshape(new_shape)


def forward(component, upper_face, dimension):
    length = component.shape[dimension]
    shifted_up = jnp.concatenate([lax.slice_in_dim(component, 1, length, axis=dimension), upper_face], axis=dimension)
    return shifted_up - component


def backward(component, lower_face, dimension):
    length = component.shape[dimension]
    behind = jnp.concatenate([lower_face, lax.slice_in_dim(component, 0, length - 1, axis=dimension)], axis=dimension)
    return component - behind


def curl(components, faces, difference):
    def slope(member, dimension):
        return difference(components[member], faces[(dimension, member)], dimension + 1)
    return [slope(2, 1) - slope(1, 2), slope(0, 2) - slope(2, 0), slope(1, 0) - slope(0, 1)]


def zero_faces(sample):
    faces = {}
    for dimension in range(3):
        face_shape = list(sample.shape)
        face_shape[dimension + 1] = 1
        for member in range(3):
            faces[(dimension, member)] = jnp.zeros(face_shape, sample.dtype)
    return faces


def reference(electric, magnetic, current, density_tiles, tile_slabs, design_box, material_mask, material_levels):
    tile_blocks = density_tiles.reshape(N_WIDE, CX // 2, NY // 2, NZ // 2)
    inverse = jnp.zeros((N_WIDE,), jnp.int32).at[tile_slabs].set(jnp.arange(N_WIDE, dtype=jnp.int32))
    coarse = jnp.take(tile_blocks, inverse, axis=0).reshape(NX // 2, NY // 2, NZ // 2)
    for dimension in range(3):
        length = coarse.shape[dimension]
        edge = lax.slice_in_dim(coarse, length - 1, length, axis=dimension)
        coarse = refine(jnp.concatenate([coarse, edge], axis=dimension), dimension)
    projected = jnp.stack([project(coarse, threshold) for threshold in thresholds])
    global_x = jnp.arange(NX, dtype=jnp.int32)
    global_y = jnp.arange(NY, dtype=jnp.int32)
    global_z = jnp.arange(NZ, dtype=jnp.int32)
    inside = (((global_x >= design_box[0]) & (global_x < design_box[1]))[:, None, None]
              & ((global_y >= design_box[2]) & (global_y < design_box[3]))[None, :, None]
              & ((global_z >= design_box[4]) & (global_z < design_box[5]))[None, None, :])
    background = jnp.where(material_mask == 1, material_levels[1], material_levels[0])
    design = material_levels[0] + projected * (material_levels[1] - material_levels[0])
    permittivity = jnp.where(inside[None], design, background[None])
    coefficient = time_step / permittivity
    faces = zero_faces(electric[:, 0])
    for iteration in range(STEPS):
        curl_e = curl([electric[:, member] for member in range(3)], faces, forward)
        magnetic = jnp.stack([magnetic[:, member] - time_step * curl_e[member] for member in range(3)], axis=1)
        curl_h = curl([magnetic[:, member] for member in range(3)], faces, backward)
        electric = jnp.stack([electric[:, member] + coefficient * (curl_h[member] - current[member]) for member in range(3)], axis=1)
    return electric, magnetic
```

```python
import functools
import math

import jax
import jax.numpy as jnp
from jax import lax
from jax.experimental import pallas as pl
from jax.experimental.pallas import tpu as pltpu
from jax.sharding import PartitionSpec as P

STEPS = 4
sharpness = 8.0
thresholds = (0.7, 0.5, 0.3)
time_step = 0.5

PAD = 8
MESH = pl.DeviceIdType.MESH
UP, DOWN, RIGHT, LEFT, DIAG_A, DIAG_B = range(6)


def refine_weights(rows, columns, offset, cells):
    k = lax.broadcasted_iota(jnp.int32, (rows, columns), 0) - offset
    j = lax.broadcasted_iota(jnp.int32, (rows, columns), 1)
    return _weights(k, j, cells)


def _weights(k, j, last):
    cell = j >> 1
    odd = (j & 1) == 1
    here = jnp.where(k == cell, jnp.where(odd, 0.5, 1.0), 0.0)
    above = jnp.where(odd & (k == jnp.minimum(cell + 1, last)), 0.5, 0.0)
    return here + above


def exact_dot(a, b):
    return jnp.dot(a, b, precision=lax.Precision.HIGHEST, preferred_element_type=jnp.float32)


def kernel(
    W,
    N,
    slabs_in,
    box_in,
    levels_in,
    e_in,
    h_in,
    j_in,
    tiles_in,
    mask_in,
    E,
    H,
    slabs,
    box,
    levels,
    J,
    tile,
    mask,
    coef,
    gathered,
    unpacked,
    coarse,
    row_send,
    row_recv,
    s_up,
    xlo,
    xhi,
    s_right,
    r_right,
    s_left,
    r_left,
    r_diag_a,
    r_diag_b,
    h_row,
    load_sem,
    send_sem,
    recv_sem,
    tile_sems,
    row_sems,
):
    w = lax.axis_index("wide")
    n = lax.axis_index("narrow")
    R, _, X, Y, Z = e_in.shape
    HY, TR, HZ = tiles_in.shape
    own_x = pl.ds(1, X)
    own_y = pl.ds(PAD, Y)

    loads = [
        pltpu.make_async_copy(tiles_in, tile, load_sem.at[0]),
        pltpu.make_async_copy(e_in, E.at[:, :, own_x, own_y, :], load_sem.at[1]),
        pltpu.make_async_copy(h_in, H.at[:, :, own_x, own_y, :], load_sem.at[2]),
        pltpu.make_async_copy(j_in, J, load_sem.at[3]),
        pltpu.make_async_copy(mask_in, mask, load_sem.at[4]),
        pltpu.make_async_copy(slabs_in, slabs, load_sem.at[5]),
        pltpu.make_async_copy(box_in, box, load_sem.at[6]),
        pltpu.make_async_copy(levels_in, levels, load_sem.at[7]),
    ]
    for load in loads:
        load.start()

    has_up = w < W - 1
    has_down = w > 0
    has_right = n < N - 1
    has_left = n > 0

    barrier = pltpu.get_barrier_semaphore()

    @pl.loop(1, W)
    def _(d):
        pl.semaphore_signal(
            barrier, inc=1, device_id=(lax.rem(w + d, W), n), device_id_type=MESH
        )

    others = (
        (has_right, w, n + 1),
        (has_left, w, n - 1),
        (has_down & has_right, w - 1, n + 1),
        (has_up & has_left, w + 1, n - 1),
    )
    expected = W - 1
    for there, to_w, to_n in others:
        expected = expected + there.astype(jnp.int32)

        @pl.when(there)
        def _():
            pl.semaphore_signal(barrier, inc=1, device_id=(to_w, to_n), device_id_type=MESH)

    zero_plane = jnp.zeros((Y + 2 * PAD, Z), jnp.float32)
    zero_tile = jnp.zeros((PAD, Z), jnp.float32)

    @pl.loop(0, R)
    def _(r):
        for c in range(3):
            E[r, c, X + 1] = zero_plane
            H[r, c, 0] = zero_plane
            for p in range(1, X + 1):
                E[r, c, p, pl.ds(PAD + Y, PAD), :] = zero_tile
                H[r, c, p, pl.ds(0, PAD), :] = zero_tile
        h_row[r] = jnp.zeros((2, X, Z), jnp.float32)

    half = TR // 2
    loads[0].wait()
    for p in range(half):
        gathered[w, pl.ds(p * HY, HY), :] = jnp.concatenate(
            [tile[:, p, :], tile[:, p + half, :]], axis=-1
        )

    pl.semaphore_wait(barrier, expected)

    def tile_copy(d):
        return pltpu.make_async_remote_copy(
            src_ref=gathered.at[w],
            dst_ref=gathered.at[w],
            send_sem=tile_sems.at[0],
            recv_sem=tile_sems.at[1],
            device_id=(lax.rem(w + d, W), n),
            device_id_type=MESH,
        )

    def messages(s, r):
        b = s % 2

        def copy(kind, src, dst, to_w, to_n):
            return pltpu.make_async_remote_copy(
                src_ref=src,
                dst_ref=dst,
                send_sem=send_sem.at[r, kind],
                recv_sem=recv_sem.at[b, r, kind],
                device_id=(to_w, to_n),
                device_id_type=MESH,
            )

        rows = 5 if s == 0 else 3
        return [
            (has_up, has_down, copy(UP, s_up.at[b, r], xlo.at[b, r], w + 1, n)),
            (
                has_down,
                has_up,
                copy(DOWN, E.at[r, pl.ds(1, 2), 1, own_y, :], xhi.at[b, r], w - 1, n),
            ),
            (
                has_right,
                has_left,
                copy(
                    RIGHT,
                    s_right.at[b, r, pl.ds(0, rows)],
                    r_right.at[b, r, pl.ds(0, rows)],
                    w,
                    n + 1,
                ),
            ),
            (has_left, has_right, copy(LEFT, s_left.at[b, r], r_left.at[b, r], w, n - 1)),
            (
                has_down & has_right,
                has_up & has_left,
                copy(
                    DIAG_A, E.at[r, 1, 1, pl.ds(Y, PAD), :], r_diag_a.at[b, r], w - 1, n + 1
                ),
            ),
            (
                has_up & has_left,
                has_down & has_right,
                copy(
                    DIAG_B, E.at[r, 0, X, pl.ds(PAD, PAD), :], r_diag_b.at[b, r], w + 1, n - 1
                ),
            ),
        ]

    last_row = lax.broadcasted_iota(jnp.int32, (Y, Z), 0) == Y - 1

    def send(s, r):
        b = s % 2
        ex, ey, ez = (E[r, c, X, own_y, :] for c in range(3))
        beyond = jnp.where(last_row, 0.0, E[r, 0, X, pl.ds(PAD + 1, Y), :])
        s_up[b, r, 0] = H[r, 1, X, own_y, :] - time_step * ((next_z(ex) - ex) + ez)
        s_up[b, r, 1] = H[r, 2, X, own_y, :] + time_step * ((beyond - ex) + ey)
        for p in range(X):
            for c in range(3):
                s_right[b, r, c, pl.ds(p, 1), :] = E[r, c, p + 1, pl.ds(PAD + Y - 1, 1), :]
            if s == 0:
                s_right[b, r, 3, pl.ds(p, 1), :] = H[r, 0, p + 1, pl.ds(PAD + Y - 1, 1), :]
                s_right[b, r, 4, pl.ds(p, 1), :] = H[r, 2, p + 1, pl.ds(PAD + Y - 1, 1), :]
            s_left[b, r, 0, pl.ds(p, 1), :] = E[r, 0, p + 1, pl.ds(PAD, 1), :]
            s_left[b, r, 1, pl.ds(p, 1), :] = E[r, 2, p + 1, pl.ds(PAD, 1), :]
        for sends, _, copy in messages(s, r):
            pl.when(sends)(copy.start)

    def receive(s, r):
        b = s % 2
        for sends, receives, copy in messages(s, r):
            pl.when(receives)(copy.wait_recv)
            pl.when(sends)(copy.wait_send)

        @pl.when(has_down)
        def _():
            H[r, 1, 0, own_y, :] = xlo[b, r, 0] + time_step * E[r, 2, 1, own_y, :]
            corner = jnp.broadcast_to(r_diag_b[b, r, pl.ds(0, 1), :], (Y, Z))
            corner = jnp.where(last_row & jnp.broadcast_to(has_right, (Y, Z)), corner, 0.0)
            H[r, 2, 0, own_y, :] = xlo[b, r, 1] + time_step * (corner - E[r, 1, 1, own_y, :])

        @pl.when(has_up)
        def _():
            E[r, 1, X + 1, own_y, :] = xhi[b, r, 0]
            E[r, 2, X + 1, own_y, :] = xhi[b, r, 1]

        @pl.when(has_right)
        def _():
            for p in range(X):
                E[r, 0, p + 1, pl.ds(PAD + Y, 1), :] = r_left[b, r, 0, pl.ds(p, 1), :]
                E[r, 2, p + 1, pl.ds(PAD + Y, 1), :] = r_left[b, r, 1, pl.ds(p, 1), :]

    def next_z(value):
        lane = lax.broadcasted_iota(jnp.int32, value.shape, 1)
        return jnp.where(lane == Z - 1, 0.0, pltpu.roll(value, Z - 1, 1))

    def last_z(value):
        lane = lax.broadcasted_iota(jnp.int32, value.shape, 1)
        return jnp.where(lane == 0, 0.0, pltpu.roll(value, 1, 1))

    def update_h(s, r):
        b = s % 2
        above = pl.ds(PAD + 1, Y)
        for p in range(1, X + 1):
            ex, ey, ez = (E[r, c, p, own_y, :] for c in range(3))
            curl_x = (E[r, 2, p, above, :] - ez) - (next_z(ey) - ey)
            curl_y = (next_z(ex) - ex) - (E[r, 2, p + 1, own_y, :] - ez)
            curl_z = (E[r, 1, p + 1, own_y, :] - ey) - (E[r, 0, p, above, :] - ex)
            for c, curl in enumerate((curl_x, curl_y, curl_z)):
                H[r, c, p, own_y, :] = H[r, c, p, own_y, :] - time_step * curl

        @pl.when(has_left)
        def _():
            ex, ey, ez = (r_right[b, r, c] for c in range(3))
            if s == 0:
                hx, hz = r_right[b, r, 3], r_right[b, r, 4]
            else:
                hx, hz = h_row[r, 0], h_row[r, 1]
            plane = lax.broadcasted_iota(jnp.int32, (X, Z), 0)
            corner = jnp.broadcast_to(r_diag_a[b, r, pl.ds(PAD - 1, 1), :], (X, Z))
            corner = jnp.where(has_up, corner, 0.0)
            ey_up = jnp.where(plane == X - 1, corner, pltpu.roll(ey, X - 1, 0))
            hx = hx - time_step * ((s_left[b, r, 1] - ez) - (next_z(ey) - ey))
            hz = hz - time_step * ((ey_up - ey) - (s_left[b, r, 0] - ex))
            h_row[r, 0] = hx
            h_row[r, 1] = hz
            for p in range(X):
                H[r, 0, p + 1, pl.ds(PAD - 1, 1), :] = h_row[r, 0, pl.ds(p, 1), :]
                H[r, 2, p + 1, pl.ds(PAD - 1, 1), :] = h_row[r, 1, pl.ds(p, 1), :]

    def update_e(r):
        below = pl.ds(PAD - 1, Y)
        for p in range(1, X + 1):
            hx, hy, hz = (H[r, c, p, own_y, :] for c in range(3))
            curl_x = (hz - H[r, 2, p, below, :]) - (hy - last_z(hy))
            curl_y = (hx - last_z(hx)) - (hz - H[r, 2, p - 1, own_y, :])
            curl_z = (hy - H[r, 1, p - 1, own_y, :]) - (hx - H[r, 0, p, below, :])
            k = coef[r, p - 1]
            for c, curl in enumerate((curl_x, curl_y, curl_z)):
                E[r, c, p, own_y, :] = E[r, c, p, own_y, :] + k * (curl - J[c, p - 1])

    @pl.loop(1, W)
    def _(d):
        tile_copy(d).start()

    loads[1].wait()
    loads[2].wait()

    @pl.loop(0, R)
    def _(r):
        send(0, r)


    loads[3].wait()
    loads[4].wait()

    others_tiles = gathered.at[pl.ds(0, W - 1)]
    for i in range(2):
        pltpu.make_async_copy(others_tiles, others_tiles, tile_sems.at[i]).wait()
    for load in loads[5:]:
        load.wait()

    mine, following = jnp.int32(0), jnp.int32(0)
    for t in range(W):
        mine = jnp.where(slabs[t] == w, t, mine)
        following = jnp.where(slabs[t] == w + 1, t, following)
    low = refine_weights(2 * HZ, Z, 0, HZ - 1)
    high = refine_weights(2 * HZ, Z, HZ, HZ - 1)
    block = gathered[mine]
    unpacked[0] = exact_dot(block, low)
    unpacked[1] = exact_dot(block, high)
    unpacked[2] = exact_dot(gathered[following], low)
    depth = coarse.shape[1]
    for p in range(TR + 1):
        coarse[p, pl.ds(HY, depth - HY), :] = jnp.zeros((depth - HY, Z), jnp.float32)
    for p in range(TR):
        coarse[p, pl.ds(0, HY), :] = unpacked[p // half, pl.ds((p % half) * HY, HY), :]
    last = unpacked[(TR - 1) // half, pl.ds(((TR - 1) % half) * HY, HY), :]
    coarse[TR, pl.ds(0, HY), :] = jnp.where(has_up, unpacked[2, pl.ds(0, HY), :], last)
    for p in range(TR + 1):
        row_send[pl.ds(p, 1), :] = coarse[p, pl.ds(0, 1), :]
    row_copy = pltpu.make_async_remote_copy(
        src_ref=row_send,
        dst_ref=row_recv,
        send_sem=row_sems.at[0],
        recv_sem=row_sems.at[1],
        device_id=(w, n - 1),
        device_id_type=MESH,
    )
    pl.when(has_left)(row_copy.start)
    pl.when(has_right)(row_copy.wait_recv)
    pl.when(has_left)(row_copy.wait_send)
    for p in range(TR + 1):

        @pl.when(has_right)
        def _():
            coarse[p, pl.ds(HY, 1), :] = row_recv[pl.ds(p, 1), :]

        @pl.when(jnp.logical_not(has_right))
        def _():
            coarse[p, pl.ds(HY, 1), :] = coarse[p, pl.ds(HY - 1, 1), :]

    fine_j = lax.broadcasted_iota(jnp.int32, (Y, depth), 0)
    coarse_k = lax.broadcasted_iota(jnp.int32, (Y, depth), 1)
    along_y = _weights(coarse_k, fine_j, HY)
    for p in range(TR + 1):
        unpacked[p] = exact_dot(along_y, coarse[p])

    level0, level1 = levels[0], levels[1]
    global_y = n * Y + lax.broadcasted_iota(jnp.int32, (Y, Z), 0)
    global_z = lax.broadcasted_iota(jnp.int32, (Y, Z), 1)
    inside_yz = (
        (global_y >= box[2]) & (global_y < box[3]) & (global_z >= box[4]) & (global_z < box[5])
    )

    @pl.loop(0, TR)
    def _(c):
        here = unpacked[c]
        for odd in range(2):
            density = 0.5 * (here + unpacked[c + 1]) if odd else here
            x = 2 * c + odd
            global_x = w * X + x
            x_inside = (global_x >= box[0]) & (global_x < box[1])
            inside = inside_yz & jnp.broadcast_to(x_inside, (Y, Z))
            background = jnp.where(mask[x] == 1, level1, level0)
            for r, threshold in enumerate(thresholds):
                low_end = math.tanh(sharpness * threshold)
                scale = low_end + math.tanh(sharpness * (1.0 - threshold))
                numer = low_end + jnp.tanh(sharpness * (density - threshold))
                design = level0 + (numer / scale) * (level1 - level0)
                coef[r, x] = time_step / jnp.where(inside, design, background)

    for s in range(STEPS):

        @pl.loop(0, R)
        def _(r):
            receive(s, r)
            update_h(s, r)
            update_e(r)
            if s < STEPS - 1:
                send(s + 1, r)


def write_out(e, h, e_out, h_out, sems):
    X, Y = e_out.shape[2:4]
    own = (slice(None), slice(None), pl.ds(1, X), pl.ds(PAD, Y), slice(None))
    copies = [
        pltpu.make_async_copy(e.at[own], e_out, sems.at[0]),
        pltpu.make_async_copy(h.at[own], h_out, sems.at[1]),
    ]
    for copy in copies:
        copy.start()
    for copy in copies:
        copy.wait()


def body(
    electric,
    magnetic,
    current,
    density_tiles,
    tile_slabs,
    design_box,
    material_mask,
    material_levels,
):
    W = lax.axis_size("wide")
    N = lax.axis_size("narrow")
    R, _, X, Y, Z = electric.shape
    TR, HY, HZ = density_tiles.shape
    f32 = jnp.float32
    hbm = pl.BlockSpec(memory_space=pl.ANY)
    vmem = pl.BlockSpec(memory_space=pltpu.VMEM)
    depth = -(-(HY + 1) // 8) * 8
    dma = pltpu.SemaphoreType.DMA
    scratch = [
        pltpu.SMEM(tile_slabs.shape, jnp.int32),
        pltpu.SMEM(design_box.shape, jnp.int32),
        pltpu.SMEM(material_levels.shape, f32),
        pltpu.VMEM((3, X, Y, Z), f32),
        pltpu.VMEM((HY, TR, HZ), f32),
        pltpu.VMEM((X, Y, Z), jnp.int32),
        pltpu.VMEM((R, X, Y, Z), f32),
        pltpu.VMEM((W, TR // 2 * HY, 2 * HZ), f32),
        pltpu.VMEM((TR + 1, Y, Z), f32),
        pltpu.VMEM((TR + 1, depth, Z), f32),
        pltpu.VMEM((8, Z), f32),
        pltpu.VMEM((8, Z), f32),
        pltpu.VMEM((2, R, 2, Y, Z), f32),
        pltpu.VMEM((2, R, 2, Y, Z), f32),
        pltpu.VMEM((2, R, 2, Y, Z), f32),
        pltpu.VMEM((2, R, 5, X, Z), f32),
        pltpu.VMEM((2, R, 5, X, Z), f32),
        pltpu.VMEM((2, R, 2, X, Z), f32),
        pltpu.VMEM((2, R, 2, X, Z), f32),
        pltpu.VMEM((2, R, PAD, Z), f32),
        pltpu.VMEM((2, R, PAD, Z), f32),
        pltpu.VMEM((R, 2, X, Z), f32),
        dma((8,)),
        dma((R, 6)),
        dma((2, R, 6)),
        dma((2,)),
        dma((2,)),
    ]
    state = pltpu.VMEM((R, 3, X + 2, Y + 2 * PAD, Z), f32)
    e, h = pl.pallas_call(
        functools.partial(kernel, W, N),
        out_shape=(state, state),
        in_specs=[hbm] * 8,
        out_specs=(vmem,) * 2,
        scratch_shapes=scratch,
        compiler_params=pltpu.CompilerParams(
            collective_id=0, has_side_effects=True, vmem_limit_bytes=56623104
        ),
        name="window",
    )(
        tile_slabs,
        design_box,
        material_levels,
        electric,
        magnetic,
        current,
        jnp.transpose(density_tiles, (1, 0, 2)),
        material_mask,
    )
    out = jax.ShapeDtypeStruct(electric.shape, f32)
    return pl.pallas_call(
        write_out,
        out_shape=(out, out),
        in_specs=[vmem] * 2,
        out_specs=(hbm,) * 2,
        scratch_shapes=[dma((2,))],
        compiler_params=pltpu.CompilerParams(vmem_limit_bytes=2**20),
        name="write_out",
    )(e, h)


def solution(mesh):
    strip = P(None, None, "wide", "narrow", None)
    return jax.shard_map(
        body,
        mesh=mesh,
        in_specs=(
            strip,
            strip,
            P(None, "wide", "narrow", None),
            P("wide", "narrow", None),
            P(),
            P(),
            P("wide", "narrow", None),
            P(),
        ),
        out_specs=(strip, strip),
        check_vma=False,
    )
```

```python
import functools
import math

import jax
import jax.numpy as jnp
from jax import lax
from jax.experimental import pallas as pl
from jax.experimental.pallas import tpu as pltpu
from jax.sharding import PartitionSpec as P

STEPS = 4
sharpness = 8.0
thresholds = (0.7, 0.5, 0.3)
time_step = 0.5

PAD = 8
MESH = pl.DeviceIdType.MESH
UP, DOWN, DIAG_A, DIAG_B, RIGHT, LEFT = range(6)


def refine_weights(rows, columns, offset, cells):
    k = lax.broadcasted_iota(jnp.int32, (rows, columns), 0) - offset
    j = lax.broadcasted_iota(jnp.int32, (rows, columns), 1)
    return _weights(k, j, cells)


def _weights(k, j, last):
    cell = j >> 1
    odd = (j & 1) == 1
    here = jnp.where(k == cell, jnp.where(odd, 0.5, 1.0), 0.0)
    above = jnp.where(odd & (k == jnp.minimum(cell + 1, last)), 0.5, 0.0)
    return here + above


def exact_dot(a, b):
    return jnp.dot(a, b, precision=lax.Precision.HIGHEST, preferred_element_type=jnp.float32)


def plane_size(devices):
    size = 1
    for divisor in range(1, devices + 1):
        if devices % divisor == 0 and divisor * divisor <= devices:
            size = divisor
    return size


def kernel(
    W,
    N,
    slabs_in,
    box_in,
    levels_in,
    e_in,
    h_in,
    j_in,
    tiles_in,
    mask_in,
    E,
    H,
    slabs,
    box,
    levels,
    J,
    tile,
    mask,
    coef,
    line,
    chosen,
    found,
    density,
    first_rows,
    s_up,
    xlo,
    xhi,
    s_right,
    r_right,
    s_left,
    r_left,
    r_diag_a,
    r_diag_b,
    h_row,
    load_sem,
    send_sem,
    recv_sem,
    tile_sems,
):
    w = lax.axis_index("wide")
    n = lax.axis_index("narrow")
    R, _, X, Y, Z = e_in.shape
    HY, TR, HZ = tiles_in.shape
    half = TR // 2
    packed = half * HY
    P_ = plane_size(W)
    L = W // P_
    g = lax.div(w, P_)
    j = lax.rem(w, P_)
    own_x = pl.ds(1, X)
    own_y = pl.ds(PAD, Y)

    loads = [
        pltpu.make_async_copy(tiles_in, tile, load_sem.at[0]),
        pltpu.make_async_copy(e_in, E.at[:, :, own_x, own_y, :], load_sem.at[1]),
        pltpu.make_async_copy(h_in, H.at[:, :, own_x, own_y, :], load_sem.at[2]),
        pltpu.make_async_copy(slabs_in, slabs, load_sem.at[3]),
        pltpu.make_async_copy(j_in, J, load_sem.at[4]),
        pltpu.make_async_copy(mask_in, mask, load_sem.at[5]),
        pltpu.make_async_copy(box_in, box, load_sem.at[6]),
        pltpu.make_async_copy(levels_in, levels, load_sem.at[7]),
    ]
    for load in loads:
        load.start()

    has_up = w < W - 1
    has_down = w > 0
    has_right = n < N - 1
    has_left = n > 0

    for l in range(L):
        line[l, pl.ds(packed, line.shape[1] - packed), :] = jnp.zeros(
            (line.shape[1] - packed, Z), jnp.float32
        )

    barrier = pltpu.get_barrier_semaphore()

    def greet(to_w, to_n):
        pl.semaphore_signal(barrier, inc=1, device_id=(to_w, to_n), device_id_type=MESH)

    def along_line(d):
        return lax.rem(g + d, L) * P_ + j

    def in_plane(d):
        return g * P_ + lax.rem(j + d, P_)

    expected = L - 1 + P_ - 1
    for d in range(1, L):
        greet(along_line(d), n)
    for d in range(1, P_):
        greet(in_plane(d), n)
    for there, to_w, to_n in (
        (has_up, w + 1, n),
        (has_down, w - 1, n),
        (has_down & has_right, w - 1, n + 1),
        (has_up & has_left, w + 1, n - 1),
    ):
        expected = expected + there.astype(jnp.int32)

        @pl.when(there)
        def _():
            greet(to_w, to_n)

    for there, to_n in ((has_right, n + 1), (has_left, n - 1)):
        expected = expected + L * there.astype(jnp.int32)

        @pl.when(there)
        def _():
            for d in range(L):
                greet(along_line(d), to_n)

    zero_plane = jnp.zeros((Y + 2 * PAD, Z), jnp.float32)
    zero_tile = jnp.zeros((PAD, Z), jnp.float32)

    @pl.loop(0, R)
    def _(r):
        for c in range(3):
            E[r, c, X + 1] = zero_plane
            H[r, c, 0] = zero_plane
            for p in range(1, X + 1):
                E[r, c, p, pl.ds(PAD + Y, PAD), :] = zero_tile
                H[r, c, p, pl.ds(0, PAD), :] = zero_tile

    rest = chosen.shape[1] - packed - HY
    for c in range(P_):
        chosen[c, pl.ds(packed + HY, rest), :] = jnp.zeros((rest, Z), jnp.float32)

    loads[0].wait()
    for p in range(half):
        rows = jnp.concatenate([tile[:, p, :], tile[:, p + half, :]], axis=-1)
        line[g, pl.ds(p * HY, HY), :] = rows
        first_rows[pl.ds(p, 1), :] = rows[0:1]

    pl.semaphore_wait(barrier, expected)

    def tile_copy(src, dst, k, to_w, to_n):
        return pltpu.make_async_remote_copy(
            src_ref=src,
            dst_ref=dst,
            send_sem=tile_sems.at[2 * k],
            recv_sem=tile_sems.at[2 * k + 1],
            device_id=(to_w, to_n),
            device_id_type=MESH,
        )

    for d in range(1, L):
        mine = line.at[g, pl.ds(0, packed)]
        tile_copy(mine, mine, 0, along_line(d), n).start()

    @pl.when(has_left)
    def _():
        for d in range(L):
            tile_copy(
                first_rows.at[pl.ds(0, half)],
                line.at[g, pl.ds(packed, half)],
                1,
                along_line(d),
                n - 1,
            ).start()

    def all_bytes(ref, k):
        return pltpu.make_async_copy(ref, ref, tile_sems.at[k])

    def copies(s, r):
        b = s % 2

        def copy(kind, src, dst, to_w, to_n):
            return pltpu.make_async_remote_copy(
                src_ref=src,
                dst_ref=dst,
                send_sem=send_sem.at[r, kind],
                recv_sem=recv_sem.at[b, r, kind],
                device_id=(to_w, to_n),
                device_id_type=MESH,
            )

        rows = 5 if s == 0 else 3
        wide = [
            (
                has_down & has_right,
                has_up & has_left,
                copy(
                    DIAG_A,
                    E.at[r, 1, 1, pl.ds(PAD + Y - 1, 1), :],
                    r_diag_a.at[b, r],
                    w - 1,
                    n + 1,
                ),
            ),
            (
                has_up & has_left,
                has_down & has_right,
                copy(
                    DIAG_B, E.at[r, 0, X, pl.ds(PAD, 1), :], r_diag_b.at[b, r], w + 1, n - 1
                ),
            ),
            (has_up, has_down, copy(UP, s_up.at[b, r], xlo.at[b, r], w + 1, n)),
            (
                has_down,
                has_up,
                copy(DOWN, E.at[r, pl.ds(1, 2), 1, own_y, :], xhi.at[b, r], w - 1, n),
            ),
        ]
        narrow = [
            (
                has_right,
                has_left,
                copy(
                    RIGHT,
                    s_right.at[b, r, pl.ds(0, rows)],
                    r_right.at[b, r, pl.ds(0, rows)],
                    w,
                    n + 1,
                ),
            ),
            (has_left, has_right, copy(LEFT, s_left.at[b, r], r_left.at[b, r], w, n - 1)),
        ]
        return wide, narrow

    def start(messages):
        for sends, _, copy in messages:
            pl.when(sends)(copy.start)

    def finish(messages):
        for sends, receives, copy in messages:
            pl.when(receives)(copy.wait_recv)
            pl.when(sends)(copy.wait_send)

    last_row = lax.broadcasted_iota(jnp.int32, (Y, Z), 0) == Y - 1

    def next_z(value):
        lane = lax.broadcasted_iota(jnp.int32, value.shape, 1)
        return jnp.where(lane == Z - 1, 0.0, pltpu.roll(value, Z - 1, 1))

    def last_z(value):
        lane = lax.broadcasted_iota(jnp.int32, value.shape, 1)
        return jnp.where(lane == 0, 0.0, pltpu.roll(value, 1, 1))

    def send_wide(s, r):
        b = s % 2
        ex, ey, ez = (E[r, c, X, own_y, :] for c in range(3))
        beyond = jnp.where(last_row, 0.0, E[r, 0, X, pl.ds(PAD + 1, Y), :])
        s_up[b, r, 0] = H[r, 1, X, own_y, :] - time_step * ((next_z(ex) - ex) + ez)
        s_up[b, r, 1] = H[r, 2, X, own_y, :] + time_step * ((beyond - ex) + ey)
        diag_a, diag_b, up, down = copies(s, r)[0]
        even = lax.rem(w, 2) == 0

        @pl.when(even)
        def _():
            start([diag_a, down, diag_b, up])

        @pl.when(jnp.logical_not(even))
        def _():
            start([diag_b, up, diag_a, down])

    def send_narrow(s, r):
        b = s % 2
        for p in range(X):
            for c in range(3):
                s_right[b, r, c, pl.ds(p, 1), :] = E[r, c, p + 1, pl.ds(PAD + Y - 1, 1), :]
            if s == 0:
                s_right[b, r, 3, pl.ds(p, 1), :] = H[r, 0, p + 1, pl.ds(PAD + Y - 1, 1), :]
                s_right[b, r, 4, pl.ds(p, 1), :] = H[r, 2, p + 1, pl.ds(PAD + Y - 1, 1), :]
            s_left[b, r, 0, pl.ds(p, 1), :] = E[r, 0, p + 1, pl.ds(PAD, 1), :]
            s_left[b, r, 1, pl.ds(p, 1), :] = E[r, 2, p + 1, pl.ds(PAD, 1), :]
        start(copies(s, r)[1])

    def receive_narrow(s, r):
        b = s % 2
        finish(copies(s, r)[1])

        @pl.when(has_right)
        def _():
            for p in range(X):
                E[r, 0, p + 1, pl.ds(PAD + Y, 1), :] = r_left[b, r, 0, pl.ds(p, 1), :]
                E[r, 2, p + 1, pl.ds(PAD + Y, 1), :] = r_left[b, r, 1, pl.ds(p, 1), :]

        @pl.when(has_left)
        def _():
            ex, ey, ez = (r_right[b, r, c] for c in range(3))
            if s == 0:
                hx, hz = r_right[b, r, 3], r_right[b, r, 4]
            else:
                hx, hz = h_row[r, 0], h_row[r, 1]
            plane = lax.broadcasted_iota(jnp.int32, (X, Z), 0)
            ey_up = jnp.where(plane == X - 1, 0.0, pltpu.roll(ey, X - 1, 0))
            h_row[r, 0] = hx - time_step * ((s_left[b, r, 1] - ez) - (next_z(ey) - ey))
            h_row[r, 1] = hz - time_step * ((ey_up - ey) - (s_left[b, r, 0] - ex))
            for p in range(X):
                H[r, 0, p + 1, pl.ds(PAD - 1, 1), :] = h_row[r, 0, pl.ds(p, 1), :]
                H[r, 2, p + 1, pl.ds(PAD - 1, 1), :] = h_row[r, 1, pl.ds(p, 1), :]

    def receive_wide(s, r):
        b = s % 2
        finish(copies(s, r)[0])

        @pl.when(has_down)
        def _():
            H[r, 1, 0, own_y, :] = xlo[b, r, 0] + time_step * E[r, 2, 1, own_y, :]
            corner = jnp.broadcast_to(r_diag_b[b, r], (Y, Z))
            corner = jnp.where(last_row & jnp.broadcast_to(has_right, (Y, Z)), corner, 0.0)
            H[r, 2, 0, own_y, :] = xlo[b, r, 1] + time_step * (corner - E[r, 1, 1, own_y, :])

        @pl.when(has_up)
        def _():
            E[r, 1, X + 1, own_y, :] = xhi[b, r, 0]
            E[r, 2, X + 1, own_y, :] = xhi[b, r, 1]

        @pl.when(has_up & has_left)
        def _():
            edge = h_row[r, 1, pl.ds(X - 1, 1), :]
            edge = edge - time_step * r_diag_a[b, r]
            h_row[r, 1, pl.ds(X - 1, 1), :] = edge
            H[r, 2, X, pl.ds(PAD - 1, 1), :] = edge

    def update_h(r, planes):
        above = pl.ds(PAD + 1, Y)
        for p in planes:
            ex, ey, ez = (E[r, c, p, own_y, :] for c in range(3))
            curl_x = (E[r, 2, p, above, :] - ez) - (next_z(ey) - ey)
            curl_y = (next_z(ex) - ex) - (E[r, 2, p + 1, own_y, :] - ez)
            curl_z = (E[r, 1, p + 1, own_y, :] - ey) - (E[r, 0, p, above, :] - ex)
            for c, curl in enumerate((curl_x, curl_y, curl_z)):
                H[r, c, p, own_y, :] = H[r, c, p, own_y, :] - time_step * curl

    def update_e(r, planes):
        below = pl.ds(PAD - 1, Y)
        for p in planes:
            hx, hy, hz = (H[r, c, p, own_y, :] for c in range(3))
            curl_x = (hz - H[r, 2, p, below, :]) - (hy - last_z(hy))
            curl_y = (hx - last_z(hx)) - (hz - H[r, 2, p - 1, own_y, :])
            curl_z = (hy - H[r, 1, p - 1, own_y, :]) - (hx - H[r, 0, p, below, :])
            k = coef[r, p - 1]
            for c, curl in enumerate((curl_x, curl_y, curl_z)):
                E[r, c, p, own_y, :] = E[r, c, p, own_y, :] + k * (curl - J[c, p - 1])

    inner_h = range(1, X)
    inner_e = range(2, X)
    edges = (1, X)

    loads[1].wait()
    loads[2].wait()

    @pl.loop(0, R)
    def _(r):
        send_wide(0, r)

    @pl.loop(0, R)
    def _(r):
        send_narrow(0, r)

    for load in loads[3:]:
        load.wait()

    if L > 1:
        for k in range(2):
            all_bytes(line.at[pl.ds(0, L - 1), pl.ds(0, packed)], k).wait()
    for there, k in ((has_left, 2), (has_right, 3)):

        @pl.when(there)
        def _():
            all_bytes(line.at[:, pl.ds(packed, half)], k).wait()

    for c in range(P_):
        a, b = jnp.int32(0), jnp.int32(0)
        for l in range(L):
            slab = slabs[l * P_ + j]
            a = jnp.where(slab == g * P_ + c, l, a)
            b = jnp.where(slab == g * P_ + c + 1, l, b)
        chosen[c, pl.ds(0, packed), :] = line[a, pl.ds(0, packed), :]
        chosen[c, pl.ds(packed, HY), :] = line[b, pl.ds(0, HY), :]
        chosen[c, pl.ds(packed + HY, half), :] = line[a, pl.ds(packed, half), :]
        chosen[c, pl.ds(packed + HY + half, 1), :] = line[b, pl.ds(packed, 1), :]
    found[j] = chosen[j]
    for d in range(1, P_):
        tile_copy(
            chosen.at[lax.rem(j + d, P_)], found.at[j], 2, in_plane(d), n
        ).start()

    @pl.loop(0, R)
    def _(r):
        receive_narrow(0, r)
        update_h(r, inner_h)

    if P_ > 1:
        for k in range(4, 6):
            all_bytes(found.at[pl.ds(0, P_ - 1)], k).wait()

    mine, following = jnp.int32(0), jnp.int32(0)
    for t in range(W):
        mine = jnp.where(slabs[t] == w, t % P_, mine)
        following = jnp.where(slabs[t] == w + 1, t % P_, following)
    total = found.shape[1]
    row = lax.broadcasted_iota(jnp.int32, (total, Z), 0)
    of_mine = (row < packed) | ((row >= packed + HY) & (row < packed + HY + half))
    block = jnp.where(of_mine, found[mine], found[following])
    refined = [
        exact_dot(block, refine_weights(2 * HZ, Z, 0, HZ - 1)),
        exact_dot(block, refine_weights(2 * HZ, Z, HZ, HZ - 1)),
    ]
    fine = lax.broadcasted_iota(jnp.int32, (Y, total), 0)
    source = lax.broadcasted_iota(jnp.int32, (Y, total), 1)
    cell = fine >> 1
    odd = (fine & 1) == 1

    def along_y(base, right):
        right = jnp.where(has_right, right, base + HY - 1)
        here = jnp.where(source == base + cell, jnp.where(odd, 0.5, 1.0), 0.0)
        next_cell = jnp.where(cell == HY - 1, right, base + cell + 1)
        return here + jnp.where(odd & (source == next_cell), 0.5, 0.0)

    weights = [along_y(p * HY, packed + HY + p) for p in range(half)]
    for p in range(TR):
        density[p] = exact_dot(weights[p % half], refined[p // half])
    beyond_last = exact_dot(along_y(packed, packed + HY + half), refined[0])
    density[TR] = jnp.where(has_up, beyond_last, density[TR - 1])

    level0, level1 = levels[0], levels[1]
    global_y = n * Y + lax.broadcasted_iota(jnp.int32, (Y, Z), 0)
    global_z = lax.broadcasted_iota(jnp.int32, (Y, Z), 1)
    inside_yz = (
        (global_y >= box[2]) & (global_y < box[3]) & (global_z >= box[4]) & (global_z < box[5])
    )

    @pl.loop(0, TR)
    def _(c):
        here = density[c]
        for odd_plane in range(2):
            value = 0.5 * (here + density[c + 1]) if odd_plane else here
            x = 2 * c + odd_plane
            global_x = w * X + x
            x_inside = (global_x >= box[0]) & (global_x < box[1])
            inside = inside_yz & jnp.broadcast_to(x_inside, (Y, Z))
            background = jnp.where(mask[x] == 1, level1, level0)
            for r, threshold in enumerate(thresholds):
                low_end = math.tanh(sharpness * threshold)
                scale = low_end + math.tanh(sharpness * (1.0 - threshold))
                numer = low_end + jnp.tanh(sharpness * (value - threshold))
                design = level0 + (numer / scale) * (level1 - level0)
                coef[r, x] = time_step / jnp.where(inside, design, background)

    for s in range(STEPS):
        if s > 0:

            @pl.loop(0, R)
            def _(r):
                receive_narrow(s, r)
                update_h(r, inner_h)
                update_e(r, inner_e)

        @pl.loop(0, R)
        def _(r):
            receive_wide(s, r)
            update_h(r, (X,))
            update_e(r, edges)
            if s < STEPS - 1:
                send_wide(s + 1, r)
                if s > 0:
                    send_narrow(s + 1, r)

        if s == 0:

            @pl.loop(0, R)
            def _(r):
                update_e(r, inner_e)
                if STEPS > 1:
                    send_narrow(1, r)


def write_out(e, h, e_out, h_out, sems):
    X, Y = e_out.shape[2:4]
    own = (slice(None), slice(None), pl.ds(1, X), pl.ds(PAD, Y), slice(None))
    copies = [
        pltpu.make_async_copy(e.at[own], e_out, sems.at[0]),
        pltpu.make_async_copy(h.at[own], h_out, sems.at[1]),
    ]
    for copy in copies:
        copy.start()
    for copy in copies:
        copy.wait()


def body(
    electric,
    magnetic,
    current,
    density_tiles,
    tile_slabs,
    design_box,
    material_mask,
    material_levels,
):
    W = lax.axis_size("wide")
    N = lax.axis_size("narrow")
    R, _, X, Y, Z = electric.shape
    TR, HY, HZ = density_tiles.shape
    f32 = jnp.float32
    hbm = pl.BlockSpec(memory_space=pl.ANY)
    vmem = pl.BlockSpec(memory_space=pltpu.VMEM)
    P_ = plane_size(W)
    L = W // P_
    half = TR // 2
    packed = half * HY
    total = -(-(packed + HY + half + 1) // 8) * 8
    dma = pltpu.SemaphoreType.DMA
    scratch = [
        pltpu.SMEM(tile_slabs.shape, jnp.int32),
        pltpu.SMEM(design_box.shape, jnp.int32),
        pltpu.SMEM(material_levels.shape, f32),
        pltpu.VMEM((3, X, Y, Z), f32),
        pltpu.VMEM((HY, TR, HZ), f32),
        pltpu.VMEM((X, Y, Z), jnp.int32),
        pltpu.VMEM((R, X, Y, Z), f32),
        pltpu.VMEM((L, -(-(packed + half) // 8) * 8, Z), f32),
        pltpu.VMEM((P_, total, Z), f32),
        pltpu.VMEM((P_, total, Z), f32),
        pltpu.VMEM((TR + 1, Y, Z), f32),
        pltpu.VMEM((8, Z), f32),
        pltpu.VMEM((2, R, 2, Y, Z), f32),
        pltpu.VMEM((2, R, 2, Y, Z), f32),
        pltpu.VMEM((2, R, 2, Y, Z), f32),
        pltpu.VMEM((2, R, 5, X, Z), f32),
        pltpu.VMEM((2, R, 5, X, Z), f32),
        pltpu.VMEM((2, R, 2, X, Z), f32),
        pltpu.VMEM((2, R, 2, X, Z), f32),
        pltpu.VMEM((2, R, 1, Z), f32),
        pltpu.VMEM((2, R, 1, Z), f32),
        pltpu.VMEM((R, 2, X, Z), f32),
        dma((8,)),
        dma((R, 6)),
        dma((2, R, 6)),
        dma((6,)),
    ]
    state = pltpu.VMEM((R, 3, X + 2, Y + 2 * PAD, Z), f32)
    e, h = pl.pallas_call(
        functools.partial(kernel, W, N),
        out_shape=(state, state),
        in_specs=[hbm] * 8,
        out_specs=(vmem,) * 2,
        scratch_shapes=scratch,
        compiler_params=pltpu.CompilerParams(
            collective_id=0, has_side_effects=True, vmem_limit_bytes=56623104
        ),
        name="window",
    )(
        tile_slabs,
        design_box,
        material_levels,
        electric,
        magnetic,
        current,
        jnp.transpose(density_tiles, (1, 0, 2)),
        material_mask,
    )
    out = jax.ShapeDtypeStruct(electric.shape, f32)
    return pl.pallas_call(
        write_out,
        out_shape=(out, out),
        in_specs=[vmem] * 2,
        out_specs=(hbm,) * 2,
        scratch_shapes=[dma((2,))],
        compiler_params=pltpu.CompilerParams(vmem_limit_bytes=2**20),
        name="write_out",
    )(e, h)


def solution(mesh):
    strip = P(None, None, "wide", "narrow", None)
    return jax.shard_map(
        body,
        mesh=mesh,
        in_specs=(
            strip,
            strip,
            P(None, "wide", "narrow", None),
            P("wide", "narrow", None),
            P(),
            P(),
            P("wide", "narrow", None),
            P(),
        ),
        out_specs=(strip, strip),
        check_vma=False,
    )
```

```python
import functools
import math

import jax
import jax.numpy as jnp
from jax import lax
from jax.experimental import pallas as pl
from jax.experimental.pallas import tpu as pltpu
from jax.sharding import PartitionSpec as P

STEPS = 4
sharpness = 8.0
thresholds = (0.7, 0.5, 0.3)
time_step = 0.5

PAD = 8
MESH = pl.DeviceIdType.MESH
UP, DIAG, DOWN, SOURCE, CORNER, RIGHT, LEFT = range(7)


def refine_weights(rows, columns, offset, cells):
    k = lax.broadcasted_iota(jnp.int32, (rows, columns), 0) - offset
    j = lax.broadcasted_iota(jnp.int32, (rows, columns), 1)
    return _weights(k, j, cells)


def _weights(k, j, last):
    cell = j >> 1
    odd = (j & 1) == 1
    here = jnp.where(k == cell, jnp.where(odd, 0.5, 1.0), 0.0)
    above = jnp.where(odd & (k == jnp.minimum(cell + 1, last)), 0.5, 0.0)
    return here + above


def exact_dot(a, b):
    return jnp.dot(a, b, precision=lax.Precision.HIGHEST, preferred_element_type=jnp.float32)


def plane_size(devices):
    size = 1
    for divisor in range(1, devices + 1):
        if devices % divisor == 0 and divisor * divisor <= devices:
            size = divisor
    return size


def kernel(
    W,
    N,
    slabs_in,
    box_in,
    levels_in,
    e_in,
    h_in,
    j_in,
    tiles_in,
    mask_in,
    E,
    H,
    slabs,
    box,
    levels,
    J,
    tile,
    mask,
    coef,
    line,
    chosen,
    found,
    density,
    first_rows,
    s_up,
    s_down,
    mask_up,
    xlo,
    xhi,
    s_right,
    r_right,
    s_left,
    r_left,
    s_corner,
    r_corner,
    h_row,
    load_sem,
    send_sem,
    up_sem,
    down_sem,
    corner_sem,
    narrow_sem,
    tile_sems,
):
    w = lax.axis_index("wide")
    n = lax.axis_index("narrow")
    R, _, X, Y, Z = e_in.shape
    HY, TR, HZ = tiles_in.shape
    half = TR // 2
    packed = half * HY
    P_ = plane_size(W)
    L = W // P_
    g = lax.div(w, P_)
    j = lax.rem(w, P_)
    own_x = pl.ds(1, X)
    own_y = pl.ds(PAD, Y)

    loads = [
        pltpu.make_async_copy(tiles_in, tile, load_sem.at[0]),
        pltpu.make_async_copy(e_in, E.at[:, :, own_x, own_y, :], load_sem.at[1]),
        pltpu.make_async_copy(h_in, H.at[:, :, own_x, own_y, :], load_sem.at[2]),
        pltpu.make_async_copy(slabs_in, slabs, load_sem.at[3]),
        pltpu.make_async_copy(j_in, J, load_sem.at[4]),
        pltpu.make_async_copy(mask_in, mask, load_sem.at[5]),
        pltpu.make_async_copy(box_in, box, load_sem.at[6]),
        pltpu.make_async_copy(levels_in, levels, load_sem.at[7]),
    ]
    for load in loads:
        load.start()

    has_up = w < W - 1
    has_down = w > 0
    has_right = n < N - 1
    has_left = n > 0

    for l in range(L):
        line[l, pl.ds(packed, line.shape[1] - packed), :] = jnp.zeros(
            (line.shape[1] - packed, Z), jnp.float32
        )

    barrier = pltpu.get_barrier_semaphore()

    def greet(to_w, to_n):
        pl.semaphore_signal(barrier, inc=1, device_id=(to_w, to_n), device_id_type=MESH)

    def along_line(d):
        return lax.rem(g + d, L) * P_ + j

    def in_plane(d):
        return g * P_ + lax.rem(j + d, P_)

    expected = L - 1 + P_ - 1
    for d in range(1, L):
        greet(along_line(d), n)
    for d in range(1, P_):
        greet(in_plane(d), n)
    for there, to_w, to_n in (
        (has_up, w + 1, n),
        (has_down, w - 1, n),
        (has_down & has_right, w - 1, n + 1),
        (has_up & has_left, w + 1, n - 1),
    ):
        expected = expected + there.astype(jnp.int32)

        @pl.when(there)
        def _():
            greet(to_w, to_n)

    for there, to_n in ((has_right, n + 1), (has_left, n - 1)):
        expected = expected + L * there.astype(jnp.int32)

        @pl.when(there)
        def _():
            for d in range(L):
                greet(along_line(d), to_n)

    zero_plane = jnp.zeros((Y + 2 * PAD, Z), jnp.float32)
    zero_tile = jnp.zeros((PAD, Z), jnp.float32)

    @pl.loop(0, R)
    def _(r):
        for c in range(3):
            E[r, c, X + 1] = zero_plane
            H[r, c, 0] = zero_plane
            for p in range(1, X + 1):
                E[r, c, p, pl.ds(PAD + Y, PAD), :] = zero_tile
                H[r, c, p, pl.ds(0, PAD), :] = zero_tile

    rest = chosen.shape[1] - packed - HY
    for c in range(P_):
        chosen[c, pl.ds(packed + HY, rest), :] = jnp.zeros((rest, Z), jnp.float32)

    loads[0].wait()
    for p in range(half):
        rows = jnp.concatenate([tile[:, p, :], tile[:, p + half, :]], axis=-1)
        line[g, pl.ds(p * HY, HY), :] = rows
        first_rows[pl.ds(p, 1), :] = rows[0:1]

    pl.semaphore_wait(barrier, expected)

    def tile_copy(src, dst, k, to_w, to_n):
        return pltpu.make_async_remote_copy(
            src_ref=src,
            dst_ref=dst,
            send_sem=tile_sems.at[2 * k],
            recv_sem=tile_sems.at[2 * k + 1],
            device_id=(to_w, to_n),
            device_id_type=MESH,
        )

    for d in range(1, L):
        mine = line.at[g, pl.ds(0, packed)]
        tile_copy(mine, mine, 0, along_line(d), n).start()

    @pl.when(has_left)
    def _():
        for d in range(L):
            tile_copy(
                first_rows.at[pl.ds(0, half)],
                line.at[g, pl.ds(packed, half)],
                1,
                along_line(d),
                n - 1,
            ).start()

    def all_bytes(ref, k):
        return pltpu.make_async_copy(ref, ref, tile_sems.at[k])

    def remote(src, dst, kind, arrived, to_w, to_n):
        return pltpu.make_async_remote_copy(
            src_ref=src,
            dst_ref=dst,
            send_sem=send_sem.at[kind],
            recv_sem=arrived,
            device_id=(to_w, to_n),
            device_id_type=MESH,
        )

    planes = pl.ds(0, 2 * Y)
    edge_row = pl.ds(2 * Y, 1)

    def up_copy(s, r):
        src, dst = s_up.at[s % 2, r, planes], xlo.at[s, r, planes]
        return remote(src, dst, UP, up_sem.at[s, r], w + 1, n)

    def diag_copy(s, r):
        src, dst = s_up.at[s % 2, r, edge_row], xlo.at[s, r, edge_row]
        return remote(src, dst, DIAG, up_sem.at[s, r], w + 1, n - 1)

    def down_copy(s, r):
        if s == 0:
            src, kind = E.at[r, pl.ds(1, 2), 1, own_y, :], DOWN
        else:
            src, kind = s_down.at[s % 2, r], SOURCE
        return remote(src, xhi.at[s, r], kind, down_sem.at[s, r], w - 1, n)

    def corner_copy(s, r):
        b = s % 2
        to_w = w - 1 if s == 0 else w
        return remote(s_corner.at[b, r], r_corner.at[b, r], CORNER, corner_sem.at[b, r], to_w, n + 1)

    def sends_corner(s):
        return has_right & (has_down if s == 0 else has_up)

    def right_copy(s, r):
        b = s % 2
        rows = pl.ds(0, 5 if s == 0 else 3)
        return remote(
            s_right.at[b, r, rows], r_right.at[b, r, rows], RIGHT, narrow_sem.at[b, r, 0], w, n + 1
        )

    def left_copy(s, r):
        b = s % 2
        return remote(s_left.at[b, r], r_left.at[b, r], LEFT, narrow_sem.at[b, r, 1], w, n - 1)

    def wait_all(there, ref, sem):
        @pl.when(there)
        def _():
            pltpu.make_async_copy(ref, ref, sem).wait()

    def finish_planes(s):
        b = s % 2
        wait_all(has_up, s_up.at[b, :, planes], send_sem.at[UP])
        wait_all(has_up & has_left, s_up.at[b, :, edge_row], send_sem.at[DIAG])
        rows = pl.ds(0, 5 if s == 0 else 3)
        wait_all(has_right, s_right.at[b, :, rows], send_sem.at[RIGHT])
        wait_all(has_left, s_left.at[b], send_sem.at[LEFT])
        if s == 0:
            wait_all(has_down, s_down.at[0], send_sem.at[DOWN])

    def finish_source(s):
        wait_all(has_down, s_down.at[s % 2], send_sem.at[SOURCE])

    def finish_corner(s):
        wait_all(sends_corner(s), s_corner.at[s % 2], send_sem.at[CORNER])

    last_row = lax.broadcasted_iota(jnp.int32, (Y, Z), 0) == Y - 1

    def next_z(value):
        lane = lax.broadcasted_iota(jnp.int32, value.shape, 1)
        return jnp.where(lane == Z - 1, 0.0, pltpu.roll(value, Z - 1, 1))

    def last_z(value):
        lane = lax.broadcasted_iota(jnp.int32, value.shape, 1)
        return jnp.where(lane == 0, 0.0, pltpu.roll(value, 1, 1))

    def send_wide(s, r):
        b = s % 2
        ex, ey, ez = (E[r, c, X, own_y, :] for c in range(3))
        beyond = jnp.where(last_row, 0.0, E[r, 0, X, pl.ds(PAD + 1, Y), :])
        s_up[b, r, edge_row, :] = E[r, 0, X, pl.ds(PAD, 1), :]
        s_up[b, r, pl.ds(0, Y), :] = H[r, 1, X, own_y, :] - time_step * ((next_z(ex) - ex) + ez)
        s_up[b, r, pl.ds(Y, Y), :] = H[r, 2, X, own_y, :] + time_step * ((beyond - ex) + ey)
        if s > 0:
            pl.when(has_up & has_left)(diag_copy(s, r).start)
            pl.when(has_up)(up_copy(s, r).start)
            return
        s_corner[b, r] = E[r, 1, 1, pl.ds(PAD + Y - 1, 1), :]
        even = lax.rem(w, 2) == 0

        def go_down():
            pl.when(sends_corner(0))(corner_copy(0, r).start)
            pl.when(has_down)(down_copy(0, r).start)

        pl.when(even)(go_down)
        pl.when(has_up & has_left)(diag_copy(s, r).start)
        pl.when(has_up)(up_copy(s, r).start)
        pl.when(jnp.logical_not(even))(go_down)

    def send_source(s, r):
        b = s % 2
        hx, hy, hz = (H[r, c, 1, own_y, :] for c in range(3))
        left_hx = H[r, 0, 1, pl.ds(PAD - 1, Y), :]
        s_down[b, r, 0] = (hx - last_z(hx)) - hz - J[1, 0]
        s_down[b, r, 1] = hy - (hx - left_hx) - J[2, 0]
        pl.when(has_down)(down_copy(s, r).start)

    def send_narrow(s, r):
        b = s % 2
        for p in range(X):
            for c in range(3):
                s_right[b, r, c, pl.ds(p, 1), :] = E[r, c, p + 1, pl.ds(PAD + Y - 1, 1), :]
            if s == 0:
                s_right[b, r, 3, pl.ds(p, 1), :] = H[r, 0, p + 1, pl.ds(PAD + Y - 1, 1), :]
                s_right[b, r, 4, pl.ds(p, 1), :] = H[r, 2, p + 1, pl.ds(PAD + Y - 1, 1), :]
            s_left[b, r, 0, pl.ds(p, 1), :] = E[r, 0, p + 1, pl.ds(PAD, 1), :]
            s_left[b, r, 1, pl.ds(p, 1), :] = E[r, 2, p + 1, pl.ds(PAD, 1), :]
        pl.when(has_right)(right_copy(s, r).start)
        pl.when(has_left)(left_copy(s, r).start)

    def receive_narrow(s, r):
        b = s % 2
        pl.when(has_left)(right_copy(s, r).wait_recv)
        pl.when(has_right)(left_copy(s, r).wait_recv)

        @pl.when(has_right)
        def _():
            for p in range(X):
                E[r, 0, p + 1, pl.ds(PAD + Y, 1), :] = r_left[b, r, 0, pl.ds(p, 1), :]
                E[r, 2, p + 1, pl.ds(PAD + Y, 1), :] = r_left[b, r, 1, pl.ds(p, 1), :]

        @pl.when(has_left)
        def _():
            ex, ey, ez = (r_right[b, r, c] for c in range(3))
            if s == 0:
                hx, hz = r_right[b, r, 3], r_right[b, r, 4]
            else:
                hx, hz = h_row[r, 0], h_row[r, 1]
            plane = lax.broadcasted_iota(jnp.int32, (X, Z), 0)
            ey_up = jnp.where(plane == X - 1, 0.0, pltpu.roll(ey, X - 1, 0))
            h_row[r, 0] = hx - time_step * ((s_left[b, r, 1] - ez) - (next_z(ey) - ey))
            h_row[r, 1] = hz - time_step * ((ey_up - ey) - (s_left[b, r, 0] - ex))
            for p in range(X):
                H[r, 0, p + 1, pl.ds(PAD - 1, 1), :] = h_row[r, 0, pl.ds(p, 1), :]
                H[r, 2, p + 1, pl.ds(PAD - 1, 1), :] = h_row[r, 1, pl.ds(p, 1), :]

    def receive_wide(s, r):
        b = s % 2
        both = pl.ds(0, 2 * Y + 1)
        wait_all(has_down & has_right, xlo.at[s, r, both], up_sem.at[s, r])
        wait_all(has_down & jnp.logical_not(has_right), xlo.at[s, r, planes], up_sem.at[s, r])
        pl.when(has_up & has_left)(corner_copy(s, r).wait_recv)

        @pl.when(has_down)
        def _():
            edge = jnp.broadcast_to(xlo[s, r, edge_row, :], (Y, Z))
            edge = jnp.where(last_row & jnp.broadcast_to(has_right, (Y, Z)), edge, 0.0)
            low_y, low_z = xlo[s, r, pl.ds(0, Y), :], xlo[s, r, pl.ds(Y, Y), :]
            H[r, 1, 0, own_y, :] = low_y + time_step * E[r, 2, 1, own_y, :]
            H[r, 2, 0, own_y, :] = low_z + time_step * (edge - E[r, 1, 1, own_y, :])

        if s == 0:

            @pl.when(has_up)
            def _():
                down_copy(0, r).wait_recv()
                E[r, 1, X + 1, own_y, :] = xhi[0, r, 0]
                E[r, 2, X + 1, own_y, :] = xhi[0, r, 1]

        @pl.when(has_up & has_left)
        def _():
            edge = h_row[r, 1, pl.ds(X - 1, 1), :] - time_step * r_corner[b, r]
            h_row[r, 1, pl.ds(X - 1, 1), :] = edge
            H[r, 2, X, pl.ds(PAD - 1, 1), :] = edge

    def receive_source(s, r):
        b = s % 2

        @pl.when(has_up)
        def _():
            down_copy(s, r).wait_recv()
            k = coef[r, X]
            hy, hz = H[r, 1, X, own_y, :], H[r, 2, X, own_y, :]
            E[r, 1, X + 1, own_y, :] = E[r, 1, X + 1, own_y, :] + k * (xhi[s, r, 0] + hz)
            E[r, 2, X + 1, own_y, :] = E[r, 2, X + 1, own_y, :] + k * (xhi[s, r, 1] - hy)

        @pl.when(sends_corner(s))
        def _():
            s_corner[b, r] = E[r, 1, X + 1, pl.ds(PAD + Y - 1, 1), :]
            corner_copy(s, r).start()

    def update_h(r, planes):
        above = pl.ds(PAD + 1, Y)
        for p in planes:
            ex, ey, ez = (E[r, c, p, own_y, :] for c in range(3))
            curl_x = (E[r, 2, p, above, :] - ez) - (next_z(ey) - ey)
            curl_y = (next_z(ex) - ex) - (E[r, 2, p + 1, own_y, :] - ez)
            curl_z = (E[r, 1, p + 1, own_y, :] - ey) - (E[r, 0, p, above, :] - ex)
            for c, curl in enumerate((curl_x, curl_y, curl_z)):
                H[r, c, p, own_y, :] = H[r, c, p, own_y, :] - time_step * curl

    def update_e(r, planes):
        below = pl.ds(PAD - 1, Y)
        for p in planes:
            hx, hy, hz = (H[r, c, p, own_y, :] for c in range(3))
            curl_x = (hz - H[r, 2, p, below, :]) - (hy - last_z(hy))
            curl_y = (hx - last_z(hx)) - (hz - H[r, 2, p - 1, own_y, :])
            curl_z = (hy - H[r, 1, p - 1, own_y, :]) - (hx - H[r, 0, p, below, :])
            k = coef[r, p - 1]
            for c, curl in enumerate((curl_x, curl_y, curl_z)):
                E[r, c, p, own_y, :] = E[r, c, p, own_y, :] + k * (curl - J[c, p - 1])

    inner_h = range(1, X)
    inner_e = range(2, X)
    edges = (1, X)

    loads[1].wait()
    loads[2].wait()

    @pl.loop(0, R)
    def _(r):
        send_wide(0, r)

    @pl.loop(0, R)
    def _(r):
        send_narrow(0, r)

    for load in loads[3:]:
        load.wait()

    @pl.loop(0, R)
    def _(r):
        receive_narrow(0, r)
        update_h(r, inner_h)

    if L > 1:
        for k in range(2):
            all_bytes(line.at[pl.ds(0, L - 1), pl.ds(0, packed)], k).wait()
    for there, k in ((has_left, 2), (has_right, 3)):

        @pl.when(there)
        def _():
            all_bytes(line.at[:, pl.ds(packed, half)], k).wait()

    for c in range(P_):
        a, b = jnp.int32(0), jnp.int32(0)
        for l in range(L):
            slab = slabs[l * P_ + j]
            a = jnp.where(slab == g * P_ + c, l, a)
            b = jnp.where(slab == g * P_ + c + 1, l, b)
        chosen[c, pl.ds(0, packed), :] = line[a, pl.ds(0, packed), :]
        chosen[c, pl.ds(packed, HY), :] = line[b, pl.ds(0, HY), :]
        chosen[c, pl.ds(packed + HY, half), :] = line[a, pl.ds(packed, half), :]
        chosen[c, pl.ds(packed + HY + half, 1), :] = line[b, pl.ds(packed, 1), :]
    found[j] = chosen[j]
    for d in range(1, P_):
        tile_copy(
            chosen.at[lax.rem(j + d, P_)], found.at[j], 2, in_plane(d), n
        ).start()

    mask_copy = pltpu.make_async_remote_copy(
        src_ref=mask.at[0],
        dst_ref=mask_up,
        send_sem=tile_sems.at[6],
        recv_sem=tile_sems.at[7],
        device_id=(w - 1, n),
        device_id_type=MESH,
    )

    if STEPS > 1:

        @pl.loop(0, R)
        def _(r):
            send_source(1, r)

    pl.when(has_down)(mask_copy.start)

    finish_planes(0)

    @pl.loop(0, R)
    def _(r):
        receive_wide(0, r)
        update_h(r, (X,))

    if P_ > 1:
        for k in range(4, 6):
            all_bytes(found.at[pl.ds(0, P_ - 1)], k).wait()

    mine, following = jnp.int32(0), jnp.int32(0)
    for t in range(W):
        mine = jnp.where(slabs[t] == w, t % P_, mine)
        following = jnp.where(slabs[t] == w + 1, t % P_, following)
    total = found.shape[1]
    row = lax.broadcasted_iota(jnp.int32, (total, Z), 0)
    of_mine = (row < packed) | ((row >= packed + HY) & (row < packed + HY + half))
    block = jnp.where(of_mine, found[mine], found[following])
    refined = [
        exact_dot(block, refine_weights(2 * HZ, Z, 0, HZ - 1)),
        exact_dot(block, refine_weights(2 * HZ, Z, HZ, HZ - 1)),
    ]
    fine = lax.broadcasted_iota(jnp.int32, (Y, total), 0)
    source = lax.broadcasted_iota(jnp.int32, (Y, total), 1)
    cell = fine >> 1
    odd = (fine & 1) == 1

    def along_y(base, right):
        right = jnp.where(has_right, right, base + HY - 1)
        here = jnp.where(source == base + cell, jnp.where(odd, 0.5, 1.0), 0.0)
        next_cell = jnp.where(cell == HY - 1, right, base + cell + 1)
        return here + jnp.where(odd & (source == next_cell), 0.5, 0.0)

    weights = [along_y(p * HY, packed + HY + p) for p in range(half)]
    for p in range(TR):
        density[p] = exact_dot(weights[p % half], refined[p // half])
    beyond_last = exact_dot(along_y(packed, packed + HY + half), refined[0])
    density[TR] = jnp.where(has_up, beyond_last, density[TR - 1])

    level0, level1 = levels[0], levels[1]
    global_y = n * Y + lax.broadcasted_iota(jnp.int32, (Y, Z), 0)
    global_z = lax.broadcasted_iota(jnp.int32, (Y, Z), 1)
    inside_yz = (
        (global_y >= box[2]) & (global_y < box[3]) & (global_z >= box[4]) & (global_z < box[5])
    )

    def coefficients(value, x, background):
        global_x = w * X + x
        x_inside = (global_x >= box[0]) & (global_x < box[1])
        inside = inside_yz & jnp.broadcast_to(x_inside, (Y, Z))
        for r, threshold in enumerate(thresholds):
            low_end = math.tanh(sharpness * threshold)
            scale = low_end + math.tanh(sharpness * (1.0 - threshold))
            numer = low_end + jnp.tanh(sharpness * (value - threshold))
            design = level0 + (numer / scale) * (level1 - level0)
            coef[r, x] = time_step / jnp.where(inside, design, background)

    def own_coefficients(value, x):
        coefficients(value, x, jnp.where(mask[x] == 1, level1, level0))

    own_coefficients(density[0], 0)
    own_coefficients(0.5 * (density[TR - 1] + density[TR]), X - 1)

    for s in range(STEPS):
        if s > 0:
            finish_source(s)

            @pl.loop(0, R)
            def _(r):
                receive_narrow(s, r)
                update_h(r, inner_h)
                if s < STEPS - 1:
                    send_source(s + 1, r)
                update_e(r, inner_e)

            finish_corner(s - 1)

            @pl.loop(0, R)
            def _(r):
                receive_source(s, r)

            finish_planes(s)

        @pl.loop(0, R)
        def _(r):
            if s > 0:
                receive_wide(s, r)
                update_h(r, (X,))
            update_e(r, edges)
            if s < STEPS - 1:
                send_wide(s + 1, r)
                if s > 0:
                    send_narrow(s + 1, r)

        if s == 0:

            @pl.loop(0, TR - 1)
            def _(c):
                own_coefficients(0.5 * (density[c] + density[c + 1]), 2 * c + 1)
                own_coefficients(density[c + 1], 2 * c + 2)

            @pl.when(has_up)
            def _():
                mask_copy.wait_recv()
                coefficients(density[TR], X, jnp.where(mask_up[...] == 1, level1, level0))

            pl.when(has_down)(mask_copy.wait_send)

            @pl.loop(0, R)
            def _(r):
                update_e(r, inner_e)
                if STEPS > 1:
                    send_narrow(1, r)

    finish_corner(STEPS - 1)


def write_out(e, h, e_out, h_out, sems):
    X, Y = e_out.shape[2:4]
    own = (slice(None), slice(None), pl.ds(1, X), pl.ds(PAD, Y), slice(None))
    copies = [
        pltpu.make_async_copy(e.at[own], e_out, sems.at[0]),
        pltpu.make_async_copy(h.at[own], h_out, sems.at[1]),
    ]
    for copy in copies:
        copy.start()
    for copy in copies:
        copy.wait()


def body(
    electric,
    magnetic,
    current,
    density_tiles,
    tile_slabs,
    design_box,
    material_mask,
    material_levels,
):
    W = lax.axis_size("wide")
    N = lax.axis_size("narrow")
    R, _, X, Y, Z = electric.shape
    TR, HY, HZ = density_tiles.shape
    f32 = jnp.float32
    hbm = pl.BlockSpec(memory_space=pl.ANY)
    vmem = pl.BlockSpec(memory_space=pltpu.VMEM)
    P_ = plane_size(W)
    L = W // P_
    half = TR // 2
    packed = half * HY
    total = -(-(packed + HY + half + 1) // 8) * 8
    dma = pltpu.SemaphoreType.DMA
    scratch = [
        pltpu.SMEM(tile_slabs.shape, jnp.int32),
        pltpu.SMEM(design_box.shape, jnp.int32),
        pltpu.SMEM(material_levels.shape, f32),
        pltpu.VMEM((3, X, Y, Z), f32),
        pltpu.VMEM((HY, TR, HZ), f32),
        pltpu.VMEM((X, Y, Z), jnp.int32),
        pltpu.VMEM((R, X + 1, Y, Z), f32),
        pltpu.VMEM((L, -(-(packed + half) // 8) * 8, Z), f32),
        pltpu.VMEM((P_, total, Z), f32),
        pltpu.VMEM((P_, total, Z), f32),
        pltpu.VMEM((TR + 1, Y, Z), f32),
        pltpu.VMEM((8, Z), f32),
        pltpu.VMEM((2, R, 2 * Y + 8, Z), f32),
        pltpu.VMEM((2, R, 2, Y, Z), f32),
        pltpu.VMEM((Y, Z), jnp.int32),
        pltpu.VMEM((STEPS, R, 2 * Y + 8, Z), f32),
        pltpu.VMEM((STEPS, R, 2, Y, Z), f32),
        pltpu.VMEM((2, R, 5, X, Z), f32),
        pltpu.VMEM((2, R, 5, X, Z), f32),
        pltpu.VMEM((2, R, 2, X, Z), f32),
        pltpu.VMEM((2, R, 2, X, Z), f32),
        pltpu.VMEM((2, R, 1, Z), f32),
        pltpu.VMEM((2, R, 1, Z), f32),
        pltpu.VMEM((R, 2, X, Z), f32),
        dma((8,)),
        dma((7,)),
        dma((STEPS, R)),
        dma((STEPS, R)),
        dma((2, R)),
        dma((2, R, 2)),
        dma((8,)),
    ]
    state = pltpu.VMEM((R, 3, X + 2, Y + 2 * PAD, Z), f32)
    e, h = pl.pallas_call(
        functools.partial(kernel, W, N),
        out_shape=(state, state),
        in_specs=[hbm] * 8,
        out_specs=(vmem,) * 2,
        scratch_shapes=scratch,
        compiler_params=pltpu.CompilerParams(
            collective_id=0, has_side_effects=True, vmem_limit_bytes=56623104
        ),
        name="window",
    )(
        tile_slabs,
        design_box,
        material_levels,
        electric,
        magnetic,
        current,
        jnp.transpose(density_tiles, (1, 0, 2)),
        material_mask,
    )
    out = jax.ShapeDtypeStruct(electric.shape, f32)
    return pl.pallas_call(
        write_out,
        out_shape=(out, out),
        in_specs=[vmem] * 2,
        out_specs=(hbm,) * 2,
        scratch_shapes=[dma((2,))],
        compiler_params=pltpu.CompilerParams(vmem_limit_bytes=2**20),
        name="write_out",
    )(e, h)


def solution(mesh):
    strip = P(None, None, "wide", "narrow", None)
    return jax.shard_map(
        body,
        mesh=mesh,
        in_specs=(
            strip,
            strip,
            P(None, "wide", "narrow", None),
            P("wide", "narrow", None),
            P(),
            P(),
            P("wide", "narrow", None),
            P(),
        ),
        out_specs=(strip, strip),
        check_vma=False,
    )
```

```python
import functools
import math

import jax
import jax.numpy as jnp
from jax import lax
from jax.experimental import pallas as pl
from jax.experimental.pallas import tpu as pltpu
from jax.sharding import PartitionSpec as P

STEPS = 4
sharpness = 8.0
thresholds = (0.7, 0.5, 0.3)
time_step = 0.5

PAD = 8
MESH = pl.DeviceIdType.MESH
UP, DIAG, DOWN, SOURCE, CORNER, RIGHT, LEFT = range(7)


def refine_weights(rows, columns, offset, cells):
    k = lax.broadcasted_iota(jnp.int32, (rows, columns), 0) - offset
    j = lax.broadcasted_iota(jnp.int32, (rows, columns), 1)
    return _weights(k, j, cells)


def _weights(k, j, last):
    cell = j >> 1
    odd = (j & 1) == 1
    here = jnp.where(k == cell, jnp.where(odd, 0.5, 1.0), 0.0)
    above = jnp.where(odd & (k == jnp.minimum(cell + 1, last)), 0.5, 0.0)
    return here + above


def exact_dot(a, b):
    return jnp.dot(a, b, precision=lax.Precision.HIGHEST, preferred_element_type=jnp.float32)


def plane_size(devices):
    size = 1
    for divisor in range(1, devices + 1):
        if devices % divisor == 0 and divisor * divisor <= devices:
            size = divisor
    return size


def kernel(
    W,
    N,
    slabs_in,
    box_in,
    levels_in,
    e_in,
    h_in,
    j_in,
    tiles_in,
    mask_in,
    E,
    H,
    slabs,
    box,
    levels,
    J,
    tile,
    mask,
    coef,
    line,
    chosen,
    found,
    density,
    first_rows,
    s_up,
    s_down,
    mask_up,
    xlo,
    xhi,
    s_right,
    r_right,
    s_left,
    r_left,
    s_corner,
    r_corner,
    h_row,
    load_sem,
    send_sem,
    up_sem,
    down_sem,
    corner_sem,
    narrow_sem,
    tile_sems,
):
    w = lax.axis_index("wide")
    n = lax.axis_index("narrow")
    R, _, X, Y, Z = e_in.shape
    HY, TR, HZ = tiles_in.shape
    half = TR // 2
    packed = half * HY
    P_ = plane_size(W)
    L = W // P_
    g = lax.div(w, P_)
    j = lax.rem(w, P_)
    own_x = pl.ds(1, X)
    own_y = pl.ds(PAD, Y)

    loads = [
        pltpu.make_async_copy(tiles_in, tile, load_sem.at[0]),
        pltpu.make_async_copy(e_in, E.at[:, :, own_x, own_y, :], load_sem.at[1]),
        pltpu.make_async_copy(h_in, H.at[:, :, own_x, own_y, :], load_sem.at[2]),
        pltpu.make_async_copy(slabs_in, slabs, load_sem.at[3]),
        pltpu.make_async_copy(j_in, J, load_sem.at[4]),
        pltpu.make_async_copy(mask_in, mask, load_sem.at[5]),
        pltpu.make_async_copy(box_in, box, load_sem.at[6]),
        pltpu.make_async_copy(levels_in, levels, load_sem.at[7]),
    ]
    for load in loads:
        load.start()

    has_up = w < W - 1
    has_down = w > 0
    has_right = n < N - 1
    has_left = n > 0

    for l in range(L):
        line[l, pl.ds(packed, line.shape[1] - packed), :] = jnp.zeros(
            (line.shape[1] - packed, Z), jnp.float32
        )

    barrier = pltpu.get_barrier_semaphore()

    def greet(to_w, to_n):
        pl.semaphore_signal(barrier, inc=1, device_id=(to_w, to_n), device_id_type=MESH)

    def along_line(d):
        return lax.rem(g + d, L) * P_ + j

    def in_plane(d):
        return g * P_ + lax.rem(j + d, P_)

    expected = L - 1 + P_ - 1
    for d in range(1, L):
        greet(along_line(d), n)
    for d in range(1, P_):
        greet(in_plane(d), n)
    for there, to_w, to_n in (
        (has_up, w + 1, n),
        (has_down, w - 1, n),
        (has_down & has_right, w - 1, n + 1),
        (has_up & has_left, w + 1, n - 1),
    ):
        expected = expected + there.astype(jnp.int32)

        @pl.when(there)
        def _():
            greet(to_w, to_n)

    for there, to_n in ((has_right, n + 1), (has_left, n - 1)):
        expected = expected + L * there.astype(jnp.int32)

        @pl.when(there)
        def _():
            for d in range(L):
                greet(along_line(d), to_n)

    zero_plane = jnp.zeros((Y + 2 * PAD, Z), jnp.float32)
    zero_tile = jnp.zeros((PAD, Z), jnp.float32)

    @pl.loop(0, R)
    def _(r):
        for c in range(3):
            E[r, c, X + 1] = zero_plane
            H[r, c, 0] = zero_plane
            for p in range(1, X + 1):
                E[r, c, p, pl.ds(PAD + Y, PAD), :] = zero_tile
                H[r, c, p, pl.ds(0, PAD), :] = zero_tile

    rest = chosen.shape[1] - packed - HY
    for c in range(P_):
        chosen[c, pl.ds(packed + HY, rest), :] = jnp.zeros((rest, Z), jnp.float32)

    loads[0].wait()
    for p in range(half):
        rows = jnp.concatenate([tile[:, p, :], tile[:, p + half, :]], axis=-1)
        line[g, pl.ds(p * HY, HY), :] = rows
        first_rows[pl.ds(p, 1), :] = rows[0:1]

    pl.semaphore_wait(barrier, expected)

    def tile_copy(src, dst, k, to_w, to_n):
        return pltpu.make_async_remote_copy(
            src_ref=src,
            dst_ref=dst,
            send_sem=tile_sems.at[2 * k],
            recv_sem=tile_sems.at[2 * k + 1],
            device_id=(to_w, to_n),
            device_id_type=MESH,
        )

    for d in range(1, L):
        mine = line.at[g, pl.ds(0, packed)]
        tile_copy(mine, mine, 0, along_line(d), n).start()

    @pl.when(has_left)
    def _():
        for d in range(L):
            tile_copy(
                first_rows.at[pl.ds(0, half)],
                line.at[g, pl.ds(packed, half)],
                1,
                along_line(d),
                n - 1,
            ).start()

    def all_bytes(ref, k):
        return pltpu.make_async_copy(ref, ref, tile_sems.at[k])

    def remote(src, dst, kind, arrived, to_w, to_n):
        return pltpu.make_async_remote_copy(
            src_ref=src,
            dst_ref=dst,
            send_sem=send_sem.at[kind],
            recv_sem=arrived,
            device_id=(to_w, to_n),
            device_id_type=MESH,
        )

    planes = pl.ds(0, 2 * Y)
    edge_row = pl.ds(2 * Y, 1)

    def up_copy(s, r):
        src, dst = s_up.at[s % 2, r, planes], xlo.at[s, r, planes]
        return remote(src, dst, UP, up_sem.at[s, r], w + 1, n)

    def diag_copy(s, r):
        src, dst = s_up.at[s % 2, r, edge_row], xlo.at[s, r, edge_row]
        return remote(src, dst, DIAG, up_sem.at[s, r], w + 1, n - 1)

    def down_copy(s, r):
        if s == 0:
            src, kind = E.at[r, pl.ds(1, 2), 1, own_y, :], DOWN
        else:
            src, kind = s_down.at[s % 2, r], SOURCE
        return remote(src, xhi.at[s, r], kind, down_sem.at[s, r], w - 1, n)

    def corner_copy(s, r):
        b = s % 2
        to_w = w - 1 if s == 0 else w
        return remote(s_corner.at[b, r], r_corner.at[b, r], CORNER, corner_sem.at[b, r], to_w, n + 1)

    def sends_corner(s):
        return has_right & (has_down if s == 0 else has_up)

    def right_copy(s, r):
        b = s % 2
        rows = pl.ds(0, 5 if s == 0 else 3)
        return remote(
            s_right.at[b, r, rows], r_right.at[b, r, rows], RIGHT, narrow_sem.at[b, r, 0], w, n + 1
        )

    def left_copy(s, r):
        b = s % 2
        return remote(s_left.at[b, r], r_left.at[b, r], LEFT, narrow_sem.at[b, r, 1], w, n - 1)

    def wait_all(there, ref, sem):
        @pl.when(there)
        def _():
            pltpu.make_async_copy(ref, ref, sem).wait()

    def finish_up(s):
        b = s % 2
        wait_all(has_up, s_up.at[b, :, planes], send_sem.at[UP])
        wait_all(has_up & has_left, s_up.at[b, :, edge_row], send_sem.at[DIAG])

    def finish_narrow(s):
        b = s % 2
        rows = pl.ds(0, 5 if s == 0 else 3)
        wait_all(has_right, s_right.at[b, :, rows], send_sem.at[RIGHT])
        wait_all(has_left, s_left.at[b], send_sem.at[LEFT])
        if s == 0:
            wait_all(has_down, s_down.at[0], send_sem.at[DOWN])

    def finish_source(s):
        wait_all(has_down, s_down.at[s % 2], send_sem.at[SOURCE])

    def finish_corner(s):
        wait_all(sends_corner(s), s_corner.at[s % 2], send_sem.at[CORNER])

    last_row = lax.broadcasted_iota(jnp.int32, (Y, Z), 0) == Y - 1

    def next_z(value):
        lane = lax.broadcasted_iota(jnp.int32, value.shape, 1)
        return jnp.where(lane == Z - 1, 0.0, pltpu.roll(value, Z - 1, 1))

    def last_z(value):
        lane = lax.broadcasted_iota(jnp.int32, value.shape, 1)
        return jnp.where(lane == 0, 0.0, pltpu.roll(value, 1, 1))

    reals = range(R)

    def send_up(s):
        b = s % 2
        for r in reals:
            ex, ey, ez = (E[r, c, X, own_y, :] for c in range(3))
            beyond = jnp.where(last_row, 0.0, E[r, 0, X, pl.ds(PAD + 1, Y), :])
            low_y = H[r, 1, X, own_y, :] - time_step * ((next_z(ex) - ex) + ez)
            low_z = H[r, 2, X, own_y, :] + time_step * ((beyond - ex) + ey)
            s_up[b, r, edge_row, :] = E[r, 0, X, pl.ds(PAD, 1), :]
            s_up[b, r, pl.ds(0, Y), :] = low_y
            s_up[b, r, pl.ds(Y, Y), :] = low_z

    def start_up(s, r):
        pl.when(has_up & has_left)(diag_copy(s, r).start)
        pl.when(has_up)(up_copy(s, r).start)

    def send_first():
        send_up(0)
        for r in reals:
            s_corner[0, r] = E[r, 1, 1, pl.ds(PAD + Y - 1, 1), :]
        even = lax.rem(w, 2) == 0

        @pl.loop(0, R)
        def _(r):
            def go_down():
                pl.when(sends_corner(0))(corner_copy(0, r).start)
                pl.when(has_down)(down_copy(0, r).start)

            pl.when(even)(go_down)
            start_up(0, r)
            pl.when(jnp.logical_not(even))(go_down)

    def send_source(s):
        b = s % 2
        for r in reals:
            hx, hy, hz = (H[r, c, 1, own_y, :] for c in range(3))
            left_hx = H[r, 0, 1, pl.ds(PAD - 1, Y), :]
            s_down[b, r, 0] = (hx - last_z(hx)) - hz - J[1, 0]
            s_down[b, r, 1] = hy - (hx - left_hx) - J[2, 0]

        @pl.when(has_down)
        def _():
            for r in reals:
                down_copy(s, r).start()

    def send_narrow(s):
        b = s % 2

        @pl.when(has_right)
        def _():
            for r in reals:
                last = pl.ds(PAD + Y - 1, 1)
                for p in range(X):
                    for c in range(3):
                        s_right[b, r, c, pl.ds(p, 1), :] = E[r, c, p + 1, last, :]
                    if s == 0:
                        s_right[b, r, 3, pl.ds(p, 1), :] = H[r, 0, p + 1, last, :]
                        s_right[b, r, 4, pl.ds(p, 1), :] = H[r, 2, p + 1, last, :]
                right_copy(s, r).start()

        @pl.when(has_left)
        def _():
            for r in reals:
                for p in range(X):
                    s_left[b, r, 0, pl.ds(p, 1), :] = E[r, 0, p + 1, pl.ds(PAD, 1), :]
                    s_left[b, r, 1, pl.ds(p, 1), :] = E[r, 2, p + 1, pl.ds(PAD, 1), :]
                left_copy(s, r).start()

    def receive_narrow(s):
        b = s % 2

        @pl.when(has_right)
        def _():
            for r in reals:
                left_copy(s, r).wait_recv()
            for r in reals:
                for p in range(X):
                    E[r, 0, p + 1, pl.ds(PAD + Y, 1), :] = r_left[b, r, 0, pl.ds(p, 1), :]
                    E[r, 2, p + 1, pl.ds(PAD + Y, 1), :] = r_left[b, r, 1, pl.ds(p, 1), :]

        @pl.when(has_left)
        def _():
            for r in reals:
                right_copy(s, r).wait_recv()
            plane = lax.broadcasted_iota(jnp.int32, (X, Z), 0)
            for r in reals:
                ex, ey, ez = (r_right[b, r, c] for c in range(3))
                if s == 0:
                    hx, hz = r_right[b, r, 3], r_right[b, r, 4]
                else:
                    hx, hz = h_row[r, 0], h_row[r, 1]
                ey_up = jnp.where(plane == X - 1, 0.0, pltpu.roll(ey, X - 1, 0))
                own_ex, own_ez = s_left[b, r, 0], s_left[b, r, 1]
                h_row[r, 0] = hx - time_step * ((own_ez - ez) - (next_z(ey) - ey))
                h_row[r, 1] = hz - time_step * ((ey_up - ey) - (own_ex - ex))
            for r in reals:
                for p in range(X):
                    H[r, 0, p + 1, pl.ds(PAD - 1, 1), :] = h_row[r, 0, pl.ds(p, 1), :]
                    H[r, 2, p + 1, pl.ds(PAD - 1, 1), :] = h_row[r, 1, pl.ds(p, 1), :]

    def receive_up(s):
        both = pl.ds(0, 2 * Y + 1)

        @pl.when(has_down & has_right)
        def _():
            for r in reals:
                ref = xlo.at[s, r, both]
                pltpu.make_async_copy(ref, ref, up_sem.at[s, r]).wait()

        @pl.when(has_down & jnp.logical_not(has_right))
        def _():
            for r in reals:
                ref = xlo.at[s, r, planes]
                pltpu.make_async_copy(ref, ref, up_sem.at[s, r]).wait()

        @pl.when(has_down)
        def _():
            for r in reals:
                edge = jnp.broadcast_to(xlo[s, r, edge_row, :], (Y, Z))
                edge = jnp.where(last_row & jnp.broadcast_to(has_right, (Y, Z)), edge, 0.0)
                low_y, low_z = xlo[s, r, pl.ds(0, Y), :], xlo[s, r, pl.ds(Y, Y), :]
                H[r, 1, 0, own_y, :] = low_y + time_step * E[r, 2, 1, own_y, :]
                H[r, 2, 0, own_y, :] = low_z + time_step * (edge - E[r, 1, 1, own_y, :])

    def receive_corner(s):
        b = s % 2

        @pl.when(has_up & has_left)
        def _():
            for r in reals:
                corner_copy(s, r).wait_recv()
            for r in reals:
                edge = h_row[r, 1, pl.ds(X - 1, 1), :] - time_step * r_corner[b, r]
                h_row[r, 1, pl.ds(X - 1, 1), :] = edge
                H[r, 2, X, pl.ds(PAD - 1, 1), :] = edge

        if s == 0:

            @pl.when(has_up)
            def _():
                for r in reals:
                    down_copy(0, r).wait_recv()
                for r in reals:
                    E[r, 1, X + 1, own_y, :] = xhi[0, r, 0]
                    E[r, 2, X + 1, own_y, :] = xhi[0, r, 1]

    def receive_source(s):
        b = s % 2

        @pl.when(has_up)
        def _():
            for r in reals:
                down_copy(s, r).wait_recv()
            for r in reals:
                k = coef[r, X]
                hy, hz = H[r, 1, X, own_y, :], H[r, 2, X, own_y, :]
                ey = E[r, 1, X + 1, own_y, :] + k * (xhi[s, r, 0] + hz)
                E[r, 1, X + 1, own_y, :] = ey
                E[r, 2, X + 1, own_y, :] = E[r, 2, X + 1, own_y, :] + k * (xhi[s, r, 1] - hy)
                s_corner[b, r] = ey[Y - 1 : Y]

        @pl.when(sends_corner(s))
        def _():
            for r in reals:
                corner_copy(s, r).start()

    def update_h(r, planes):
        above = pl.ds(PAD + 1, Y)
        for p in planes:
            ex, ey, ez = (E[r, c, p, own_y, :] for c in range(3))
            curl_x = (E[r, 2, p, above, :] - ez) - (next_z(ey) - ey)
            curl_y = (next_z(ex) - ex) - (E[r, 2, p + 1, own_y, :] - ez)
            curl_z = (E[r, 1, p + 1, own_y, :] - ey) - (E[r, 0, p, above, :] - ex)
            for c, curl in enumerate((curl_x, curl_y, curl_z)):
                H[r, c, p, own_y, :] = H[r, c, p, own_y, :] - time_step * curl

    def update_e(r, planes):
        below = pl.ds(PAD - 1, Y)
        for p in planes:
            hx, hy, hz = (H[r, c, p, own_y, :] for c in range(3))
            curl_x = (hz - H[r, 2, p, below, :]) - (hy - last_z(hy))
            curl_y = (hx - last_z(hx)) - (hz - H[r, 2, p - 1, own_y, :])
            curl_z = (hy - H[r, 1, p - 1, own_y, :]) - (hx - H[r, 0, p, below, :])
            k = coef[r, p - 1]
            for c, curl in enumerate((curl_x, curl_y, curl_z)):
                E[r, c, p, own_y, :] = E[r, c, p, own_y, :] + k * (curl - J[c, p - 1])

    inner_h = range(1, X)
    inner_e = range(2, X)

    loads[1].wait()
    loads[2].wait()

    send_first()
    send_narrow(0)

    for load in loads[3:]:
        load.wait()

    receive_narrow(0)
    for r in reals:
        update_h(r, inner_h)

    if L > 1:
        for k in range(2):
            all_bytes(line.at[pl.ds(0, L - 1), pl.ds(0, packed)], k).wait()
    for there, k in ((has_left, 2), (has_right, 3)):

        @pl.when(there)
        def _():
            all_bytes(line.at[:, pl.ds(packed, half)], k).wait()

    for c in range(P_):
        a, b = jnp.int32(0), jnp.int32(0)
        for l in range(L):
            slab = slabs[l * P_ + j]
            a = jnp.where(slab == g * P_ + c, l, a)
            b = jnp.where(slab == g * P_ + c + 1, l, b)
        chosen[c, pl.ds(0, packed), :] = line[a, pl.ds(0, packed), :]
        chosen[c, pl.ds(packed, HY), :] = line[b, pl.ds(0, HY), :]
        chosen[c, pl.ds(packed + HY, half), :] = line[a, pl.ds(packed, half), :]
        chosen[c, pl.ds(packed + HY + half, 1), :] = line[b, pl.ds(packed, 1), :]
    found[j] = chosen[j]
    for d in range(1, P_):
        tile_copy(
            chosen.at[lax.rem(j + d, P_)], found.at[j], 2, in_plane(d), n
        ).start()

    mask_copy = pltpu.make_async_remote_copy(
        src_ref=mask.at[0],
        dst_ref=mask_up,
        send_sem=tile_sems.at[6],
        recv_sem=tile_sems.at[7],
        device_id=(w - 1, n),
        device_id_type=MESH,
    )

    if STEPS > 1:
        send_source(1)

    pl.when(has_down)(mask_copy.start)

    finish_up(0)
    finish_narrow(0)

    receive_corner(0)
    for r in reals:
        update_h(r, (X,))
    receive_up(0)

    if P_ > 1:
        for k in range(4, 6):
            all_bytes(found.at[pl.ds(0, P_ - 1)], k).wait()

    mine, following = jnp.int32(0), jnp.int32(0)
    for t in range(W):
        mine = jnp.where(slabs[t] == w, t % P_, mine)
        following = jnp.where(slabs[t] == w + 1, t % P_, following)
    total = found.shape[1]
    row = lax.broadcasted_iota(jnp.int32, (total, Z), 0)
    of_mine = (row < packed) | ((row >= packed + HY) & (row < packed + HY + half))
    block = jnp.where(of_mine, found[mine], found[following])
    refined = [
        exact_dot(block, refine_weights(2 * HZ, Z, 0, HZ - 1)),
        exact_dot(block, refine_weights(2 * HZ, Z, HZ, HZ - 1)),
    ]
    fine = lax.broadcasted_iota(jnp.int32, (Y, total), 0)
    source = lax.broadcasted_iota(jnp.int32, (Y, total), 1)
    cell = fine >> 1
    odd = (fine & 1) == 1

    def along_y(base, right):
        right = jnp.where(has_right, right, base + HY - 1)
        here = jnp.where(source == base + cell, jnp.where(odd, 0.5, 1.0), 0.0)
        next_cell = jnp.where(cell == HY - 1, right, base + cell + 1)
        return here + jnp.where(odd & (source == next_cell), 0.5, 0.0)

    weights = [along_y(p * HY, packed + HY + p) for p in range(half)]
    for p in range(TR):
        density[p] = exact_dot(weights[p % half], refined[p // half])
    beyond_last = exact_dot(along_y(packed, packed + HY + half), refined[0])
    density[TR] = jnp.where(has_up, beyond_last, density[TR - 1])

    level0, level1 = levels[0], levels[1]
    global_y = n * Y + lax.broadcasted_iota(jnp.int32, (Y, Z), 0)
    global_z = lax.broadcasted_iota(jnp.int32, (Y, Z), 1)
    inside_yz = (
        (global_y >= box[2]) & (global_y < box[3]) & (global_z >= box[4]) & (global_z < box[5])
    )

    def coefficients(value, x, background):
        global_x = w * X + x
        x_inside = (global_x >= box[0]) & (global_x < box[1])
        inside = inside_yz & jnp.broadcast_to(x_inside, (Y, Z))
        for r, threshold in enumerate(thresholds):
            low_end = math.tanh(sharpness * threshold)
            scale = low_end + math.tanh(sharpness * (1.0 - threshold))
            numer = low_end + jnp.tanh(sharpness * (value - threshold))
            design = level0 + (numer / scale) * (level1 - level0)
            coef[r, x] = time_step / jnp.where(inside, design, background)

    def own_coefficients(value, x):
        coefficients(value, x, jnp.where(mask[x] == 1, level1, level0))

    own_coefficients(0.5 * (density[TR - 1] + density[TR]), X - 1)

    def update_top(s):
        if s > 0:
            receive_corner(s)
            for r in reals:
                update_h(r, (X,))
        for r in reals:
            update_e(r, (X,))
        if s < STEPS - 1:
            send_up(s + 1)
            for r in reals:
                start_up(s + 1, r)

    update_top(0)

    own_coefficients(density[0], 0)
    for c in range(TR - 1):
        own_coefficients(0.5 * (density[c] + density[c + 1]), 2 * c + 1)
        own_coefficients(density[c + 1], 2 * c + 2)
    for r in reals:
        update_e(r, range(1, X))
    if STEPS > 1:
        send_narrow(1)

    @pl.when(has_up)
    def _():
        mask_copy.wait_recv()
        coefficients(density[TR], X, jnp.where(mask_up[...] == 1, level1, level0))

    pl.when(has_down)(mask_copy.wait_send)

    for s in range(1, STEPS):
        finish_source(s)
        receive_narrow(s)
        for r in reals:
            update_h(r, (1,))
        if s < STEPS - 1:
            send_source(s + 1)
        for r in reals:
            update_h(r, range(2, X))
        for r in reals:
            update_e(r, inner_e)
        finish_corner(s - 1)
        receive_source(s)
        finish_up(s)
        update_top(s)
        finish_narrow(s)
        receive_up(s)
        for r in reals:
            update_e(r, (1,))
        if s < STEPS - 1:
            send_narrow(s + 1)

    finish_corner(STEPS - 1)


def write_out(e, h, e_out, h_out, sems):
    X, Y = e_out.shape[2:4]
    own = (slice(None), slice(None), pl.ds(1, X), pl.ds(PAD, Y), slice(None))
    copies = [
        pltpu.make_async_copy(e.at[own], e_out, sems.at[0]),
        pltpu.make_async_copy(h.at[own], h_out, sems.at[1]),
    ]
    for copy in copies:
        copy.start()
    for copy in copies:
        copy.wait()


def body(
    electric,
    magnetic,
    current,
    density_tiles,
    tile_slabs,
    design_box,
    material_mask,
    material_levels,
):
    W = lax.axis_size("wide")
    N = lax.axis_size("narrow")
    R, _, X, Y, Z = electric.shape
    TR, HY, HZ = density_tiles.shape
    f32 = jnp.float32
    hbm = pl.BlockSpec(memory_space=pl.ANY)
    vmem = pl.BlockSpec(memory_space=pltpu.VMEM)
    P_ = plane_size(W)
    L = W // P_
    half = TR // 2
    packed = half * HY
    total = -(-(packed + HY + half + 1) // 8) * 8
    dma = pltpu.SemaphoreType.DMA
    scratch = [
        pltpu.SMEM(tile_slabs.shape, jnp.int32),
        pltpu.SMEM(design_box.shape, jnp.int32),
        pltpu.SMEM(material_levels.shape, f32),
        pltpu.VMEM((3, X, Y, Z), f32),
        pltpu.VMEM((HY, TR, HZ), f32),
        pltpu.VMEM((X, Y, Z), jnp.int32),
        pltpu.VMEM((R, X + 1, Y, Z), f32),
        pltpu.VMEM((L, -(-(packed + half) // 8) * 8, Z), f32),
        pltpu.VMEM((P_, total, Z), f32),
        pltpu.VMEM((P_, total, Z), f32),
        pltpu.VMEM((TR + 1, Y, Z), f32),
        pltpu.VMEM((8, Z), f32),
        pltpu.VMEM((2, R, 2 * Y + 8, Z), f32),
        pltpu.VMEM((2, R, 2, Y, Z), f32),
        pltpu.VMEM((Y, Z), jnp.int32),
        pltpu.VMEM((STEPS, R, 2 * Y + 8, Z), f32),
        pltpu.VMEM((STEPS, R, 2, Y, Z), f32),
        pltpu.VMEM((2, R, 5, X, Z), f32),
        pltpu.VMEM((2, R, 5, X, Z), f32),
        pltpu.VMEM((2, R, 2, X, Z), f32),
        pltpu.VMEM((2, R, 2, X, Z), f32),
        pltpu.VMEM((2, R, 1, Z), f32),
        pltpu.VMEM((2, R, 1, Z), f32),
        pltpu.VMEM((R, 2, X, Z), f32),
        dma((8,)),
        dma((7,)),
        dma((STEPS, R)),
        dma((STEPS, R)),
        dma((2, R)),
        dma((2, R, 2)),
        dma((8,)),
    ]
    state = pltpu.VMEM((R, 3, X + 2, Y + 2 * PAD, Z), f32)
    e, h = pl.pallas_call(
        functools.partial(kernel, W, N),
        out_shape=(state, state),
        in_specs=[hbm] * 8,
        out_specs=(vmem,) * 2,
        scratch_shapes=scratch,
        compiler_params=pltpu.CompilerParams(
            collective_id=0, has_side_effects=True, vmem_limit_bytes=56623104
        ),
        name="window",
    )(
        tile_slabs,
        design_box,
        material_levels,
        electric,
        magnetic,
        current,
        jnp.transpose(density_tiles, (1, 0, 2)),
        material_mask,
    )
    out = jax.ShapeDtypeStruct(electric.shape, f32)
    return pl.pallas_call(
        write_out,
        out_shape=(out, out),
        in_specs=[vmem] * 2,
        out_specs=(hbm,) * 2,
        scratch_shapes=[dma((2,))],
        compiler_params=pltpu.CompilerParams(vmem_limit_bytes=2**20),
        name="write_out",
    )(e, h)


def solution(mesh):
    strip = P(None, None, "wide", "narrow", None)
    return jax.shard_map(
        body,
        mesh=mesh,
        in_specs=(
            strip,
            strip,
            P(None, "wide", "narrow", None),
            P("wide", "narrow", None),
            P(),
            P(),
            P("wide", "narrow", None),
            P(),
        ),
        out_specs=(strip, strip),
        check_vma=False,
    )
```

```python
import functools
import math

import jax
import jax.numpy as jnp
from jax import lax
from jax.experimental import pallas as pl
from jax.experimental.pallas import tpu as pltpu
from jax.sharding import PartitionSpec as P

STEPS = 4
sharpness = 8.0
thresholds = (0.7, 0.5, 0.3)
time_step = 0.5

PAD = 8
MESH = pl.DeviceIdType.MESH
UP, DIAG, DOWN, SOURCE, CORNER, RIGHT, LEFT = range(7)


def refine_weights(rows, columns, offset, cells):
    k = lax.broadcasted_iota(jnp.int32, (rows, columns), 0) - offset
    j = lax.broadcasted_iota(jnp.int32, (rows, columns), 1)
    return _weights(k, j, cells)


def _weights(k, j, last):
    cell = j >> 1
    odd = (j & 1) == 1
    here = jnp.where(k == cell, jnp.where(odd, 0.5, 1.0), 0.0)
    above = jnp.where(odd & (k == jnp.minimum(cell + 1, last)), 0.5, 0.0)
    return here + above


def exact_dot(a, b):
    return jnp.dot(a, b, precision=lax.Precision.HIGHEST, preferred_element_type=jnp.float32)


def plane_size(devices):
    size = 1
    for divisor in range(1, devices + 1):
        if devices % divisor == 0 and divisor * divisor <= devices:
            size = divisor
    return size


def kernel(
    W,
    N,
    slabs_in,
    box_in,
    levels_in,
    e_in,
    h_in,
    j_in,
    tiles_in,
    mask_in,
    E,
    H,
    slabs,
    box,
    levels,
    J,
    tile,
    mask,
    coef,
    line,
    chosen,
    found,
    density,
    first_rows,
    s_up,
    s_down,
    mask_up,
    xlo,
    xhi,
    s_right,
    r_right,
    s_left,
    r_left,
    s_corner,
    r_corner,
    h_row,
    load_sem,
    send_sem,
    up_sem,
    down_sem,
    corner_sem,
    narrow_sem,
    tile_sems,
):
    w = lax.axis_index("wide")
    n = lax.axis_index("narrow")
    R, _, X, Y, Z = e_in.shape
    HY, TR, HZ = tiles_in.shape
    half = TR // 2
    packed = half * HY
    P_ = plane_size(W)
    L = W // P_
    g = lax.div(w, P_)
    j = lax.rem(w, P_)
    own_x = pl.ds(1, X)
    own_y = pl.ds(PAD, Y)

    loads = [
        pltpu.make_async_copy(tiles_in, tile, load_sem.at[0]),
        pltpu.make_async_copy(e_in, E.at[:, :, own_x, own_y, :], load_sem.at[1]),
        pltpu.make_async_copy(h_in, H.at[:, :, own_x, own_y, :], load_sem.at[2]),
        pltpu.make_async_copy(slabs_in, slabs, load_sem.at[3]),
        pltpu.make_async_copy(j_in, J, load_sem.at[4]),
        pltpu.make_async_copy(mask_in, mask, load_sem.at[5]),
        pltpu.make_async_copy(box_in, box, load_sem.at[6]),
        pltpu.make_async_copy(levels_in, levels, load_sem.at[7]),
    ]

    has_up = w < W - 1
    has_down = w > 0
    has_right = n < N - 1
    has_left = n > 0

    for l in range(L):
        line[l, pl.ds(packed, line.shape[1] - packed), :] = jnp.zeros(
            (line.shape[1] - packed, Z), jnp.float32
        )

    loads[0].start()
    barrier = pltpu.get_barrier_semaphore()

    def greet(to_w, to_n):
        pl.semaphore_signal(barrier, inc=1, device_id=(to_w, to_n), device_id_type=MESH)

    def along_line(d):
        return lax.rem(g + d, L) * P_ + j

    def in_plane(d):
        return g * P_ + lax.rem(j + d, P_)

    expected = L - 1 + P_ - 1
    for d in range(1, L):
        greet(along_line(d), n)
    for d in range(1, P_):
        greet(in_plane(d), n)
    for there, to_w, to_n in (
        (has_up, w + 1, n),
        (has_down, w - 1, n),
        (has_down & has_right, w - 1, n + 1),
        (has_up & has_left, w + 1, n - 1),
    ):
        expected = expected + there.astype(jnp.int32)

        @pl.when(there)
        def _():
            greet(to_w, to_n)

    for there, to_n in ((has_right, n + 1), (has_left, n - 1)):
        expected = expected + L * there.astype(jnp.int32)

        @pl.when(there)
        def _():
            for d in range(L):
                greet(along_line(d), to_n)

    for load in loads[1:]:
        load.start()

    zero_plane = jnp.zeros((Y + 2 * PAD, Z), jnp.float32)
    zero_tile = jnp.zeros((PAD, Z), jnp.float32)

    @pl.loop(0, R)
    def _(r):
        for c in range(3):
            E[r, c, X + 1] = zero_plane
            H[r, c, 0] = zero_plane
            for p in range(1, X + 1):
                E[r, c, p, pl.ds(PAD + Y, PAD), :] = zero_tile
                H[r, c, p, pl.ds(0, PAD), :] = zero_tile

    rest = chosen.shape[1] - packed - HY
    for c in range(P_):
        chosen[c, pl.ds(packed + HY, rest), :] = jnp.zeros((rest, Z), jnp.float32)

    loads[0].wait()
    for p in range(half):
        rows = jnp.concatenate([tile[:, p, :], tile[:, p + half, :]], axis=-1)
        line[g, pl.ds(p * HY, HY), :] = rows
        first_rows[pl.ds(p, 1), :] = rows[0:1]

    pl.semaphore_wait(barrier, expected)

    def tile_copy(src, dst, k, to_w, to_n):
        return pltpu.make_async_remote_copy(
            src_ref=src,
            dst_ref=dst,
            send_sem=tile_sems.at[2 * k],
            recv_sem=tile_sems.at[2 * k + 1],
            device_id=(to_w, to_n),
            device_id_type=MESH,
        )

    for d in range(1, L):
        mine = line.at[g, pl.ds(0, packed)]
        tile_copy(mine, mine, 0, along_line(d), n).start()

    @pl.when(has_left)
    def _():
        for d in range(L):
            tile_copy(
                first_rows.at[pl.ds(0, half)],
                line.at[g, pl.ds(packed, half)],
                1,
                along_line(d),
                n - 1,
            ).start()

    def all_bytes(ref, k):
        return pltpu.make_async_copy(ref, ref, tile_sems.at[k])

    def remote(src, dst, kind, arrived, to_w, to_n):
        return pltpu.make_async_remote_copy(
            src_ref=src,
            dst_ref=dst,
            send_sem=send_sem.at[kind],
            recv_sem=arrived,
            device_id=(to_w, to_n),
            device_id_type=MESH,
        )

    planes = pl.ds(0, 2 * Y)
    edge_row = pl.ds(2 * Y, 1)

    def up_copy(s, r):
        src, dst = s_up.at[s % 2, r, planes], xlo.at[s, r, planes]
        return remote(src, dst, UP, up_sem.at[s, r], w + 1, n)

    def diag_copy(s, r):
        src, dst = s_up.at[s % 2, r, edge_row], xlo.at[s, r, edge_row]
        return remote(src, dst, DIAG, up_sem.at[s, r], w + 1, n - 1)

    def down_copy(s, r):
        if s == 0:
            src, kind = E.at[r, pl.ds(1, 2), 1, own_y, :], DOWN
        else:
            src, kind = s_down.at[s % 2, r], SOURCE
        return remote(src, xhi.at[s, r], kind, down_sem.at[s, r], w - 1, n)

    def corner_copy(s, r):
        b = s % 2
        to_w = w - 1 if s == 0 else w
        return remote(s_corner.at[b, r], r_corner.at[b, r], CORNER, corner_sem.at[b, r], to_w, n + 1)

    def sends_corner(s):
        return has_right & (has_down if s == 0 else has_up)

    def right_copy(s, r):
        b = s % 2
        rows = pl.ds(0, 5 if s == 0 else 3)
        return remote(
            s_right.at[b, r, rows], r_right.at[b, r, rows], RIGHT, narrow_sem.at[b, r, 0], w, n + 1
        )

    def left_copy(s, r):
        b = s % 2
        return remote(s_left.at[b, r], r_left.at[b, r], LEFT, narrow_sem.at[b, r, 1], w, n - 1)

    def wait_all(there, ref, sem):
        @pl.when(there)
        def _():
            pltpu.make_async_copy(ref, ref, sem).wait()

    def finish_up(s):
        b = s % 2
        wait_all(has_up, s_up.at[b, :, planes], send_sem.at[UP])
        wait_all(has_up & has_left, s_up.at[b, :, edge_row], send_sem.at[DIAG])

    def finish_narrow(s):
        b = s % 2
        rows = pl.ds(0, 5 if s == 0 else 3)
        wait_all(has_right, s_right.at[b, :, rows], send_sem.at[RIGHT])
        wait_all(has_left, s_left.at[b], send_sem.at[LEFT])
        if s == 0:
            wait_all(has_down, s_down.at[0], send_sem.at[DOWN])

    def finish_source(s):
        wait_all(has_down, s_down.at[s % 2], send_sem.at[SOURCE])

    def finish_corner(s):
        wait_all(sends_corner(s), s_corner.at[s % 2], send_sem.at[CORNER])

    last_row = lax.broadcasted_iota(jnp.int32, (Y, Z), 0) == Y - 1

    def next_z(value):
        lane = lax.broadcasted_iota(jnp.int32, value.shape, 1)
        return jnp.where(lane == Z - 1, 0.0, pltpu.roll(value, Z - 1, 1))

    def last_z(value):
        lane = lax.broadcasted_iota(jnp.int32, value.shape, 1)
        return jnp.where(lane == 0, 0.0, pltpu.roll(value, 1, 1))

    reals = range(R)

    def send_up(s):
        b = s % 2
        for r in reals:
            ex, ey, ez = (E[r, c, X, own_y, :] for c in range(3))
            beyond = jnp.where(last_row, 0.0, E[r, 0, X, pl.ds(PAD + 1, Y), :])
            low_y = H[r, 1, X, own_y, :] - time_step * ((next_z(ex) - ex) + ez)
            low_z = H[r, 2, X, own_y, :] + time_step * ((beyond - ex) + ey)
            s_up[b, r, edge_row, :] = E[r, 0, X, pl.ds(PAD, 1), :]
            s_up[b, r, pl.ds(0, Y), :] = low_y
            s_up[b, r, pl.ds(Y, Y), :] = low_z

    def start_up(s, r):
        pl.when(has_up & has_left)(diag_copy(s, r).start)
        pl.when(has_up)(up_copy(s, r).start)

    def send_first():
        send_up(0)
        for r in reals:
            s_corner[0, r] = E[r, 1, 1, pl.ds(PAD + Y - 1, 1), :]
        even = lax.rem(w, 2) == 0

        @pl.loop(0, R)
        def _(r):
            def go_down():
                pl.when(sends_corner(0))(corner_copy(0, r).start)
                pl.when(has_down)(down_copy(0, r).start)

            pl.when(even)(go_down)
            start_up(0, r)
            pl.when(jnp.logical_not(even))(go_down)

    def send_source(s):
        b = s % 2
        for r in reals:
            hx, hy, hz = (H[r, c, 1, own_y, :] for c in range(3))
            left_hx = H[r, 0, 1, pl.ds(PAD - 1, Y), :]
            s_down[b, r, 0] = (hx - last_z(hx)) - hz - J[1, 0]
            s_down[b, r, 1] = hy - (hx - left_hx) - J[2, 0]

        @pl.when(has_down)
        def _():
            for r in reals:
                down_copy(s, r).start()

    def send_narrow(s):
        b = s % 2

        @pl.when(has_right)
        def _():
            for r in reals:
                last = pl.ds(PAD + Y - 1, 1)
                for p in range(X):
                    for c in range(3):
                        s_right[b, r, c, pl.ds(p, 1), :] = E[r, c, p + 1, last, :]
                    if s == 0:
                        s_right[b, r, 3, pl.ds(p, 1), :] = H[r, 0, p + 1, last, :]
                        s_right[b, r, 4, pl.ds(p, 1), :] = H[r, 2, p + 1, last, :]
                right_copy(s, r).start()

        @pl.when(has_left)
        def _():
            for r in reals:
                for p in range(X):
                    s_left[b, r, 0, pl.ds(p, 1), :] = E[r, 0, p + 1, pl.ds(PAD, 1), :]
                    s_left[b, r, 1, pl.ds(p, 1), :] = E[r, 2, p + 1, pl.ds(PAD, 1), :]
                left_copy(s, r).start()

    def receive_narrow(s):
        b = s % 2

        @pl.when(has_right)
        def _():
            for r in reals:
                left_copy(s, r).wait_recv()
            for r in reals:
                for p in range(X):
                    E[r, 0, p + 1, pl.ds(PAD + Y, 1), :] = r_left[b, r, 0, pl.ds(p, 1), :]
                    E[r, 2, p + 1, pl.ds(PAD + Y, 1), :] = r_left[b, r, 1, pl.ds(p, 1), :]

        @pl.when(has_left)
        def _():
            for r in reals:
                right_copy(s, r).wait_recv()
            plane = lax.broadcasted_iota(jnp.int32, (X, Z), 0)
            for r in reals:
                ex, ey, ez = (r_right[b, r, c] for c in range(3))
                if s == 0:
                    hx, hz = r_right[b, r, 3], r_right[b, r, 4]
                else:
                    hx, hz = h_row[r, 0], h_row[r, 1]
                ey_up = jnp.where(plane == X - 1, 0.0, pltpu.roll(ey, X - 1, 0))
                own_ex, own_ez = s_left[b, r, 0], s_left[b, r, 1]
                h_row[r, 0] = hx - time_step * ((own_ez - ez) - (next_z(ey) - ey))
                h_row[r, 1] = hz - time_step * ((ey_up - ey) - (own_ex - ex))
            for r in reals:
                for p in range(X):
                    H[r, 0, p + 1, pl.ds(PAD - 1, 1), :] = h_row[r, 0, pl.ds(p, 1), :]
                    H[r, 2, p + 1, pl.ds(PAD - 1, 1), :] = h_row[r, 1, pl.ds(p, 1), :]

    def receive_up(s):
        both = pl.ds(0, 2 * Y + 1)

        @pl.when(has_down & has_right)
        def _():
            for r in reals:
                ref = xlo.at[s, r, both]
                pltpu.make_async_copy(ref, ref, up_sem.at[s, r]).wait()

        @pl.when(has_down & jnp.logical_not(has_right))
        def _():
            for r in reals:
                ref = xlo.at[s, r, planes]
                pltpu.make_async_copy(ref, ref, up_sem.at[s, r]).wait()

        @pl.when(has_down)
        def _():
            for r in reals:
                edge = jnp.broadcast_to(xlo[s, r, edge_row, :], (Y, Z))
                edge = jnp.where(last_row & jnp.broadcast_to(has_right, (Y, Z)), edge, 0.0)
                low_y, low_z = xlo[s, r, pl.ds(0, Y), :], xlo[s, r, pl.ds(Y, Y), :]
                H[r, 1, 0, own_y, :] = low_y + time_step * E[r, 2, 1, own_y, :]
                H[r, 2, 0, own_y, :] = low_z + time_step * (edge - E[r, 1, 1, own_y, :])

    def receive_corner(s):
        b = s % 2

        @pl.when(has_up & has_left)
        def _():
            for r in reals:
                corner_copy(s, r).wait_recv()
            for r in reals:
                edge = h_row[r, 1, pl.ds(X - 1, 1), :] - time_step * r_corner[b, r]
                h_row[r, 1, pl.ds(X - 1, 1), :] = edge
                H[r, 2, X, pl.ds(PAD - 1, 1), :] = edge

        if s == 0:

            @pl.when(has_up)
            def _():
                for r in reals:
                    down_copy(0, r).wait_recv()
                for r in reals:
                    E[r, 1, X + 1, own_y, :] = xhi[0, r, 0]
                    E[r, 2, X + 1, own_y, :] = xhi[0, r, 1]

    def receive_source(s):
        b = s % 2

        @pl.when(has_up)
        def _():
            for r in reals:
                down_copy(s, r).wait_recv()
            for r in reals:
                k = coef[r, X]
                hy, hz = H[r, 1, X, own_y, :], H[r, 2, X, own_y, :]
                ey = E[r, 1, X + 1, own_y, :] + k * (xhi[s, r, 0] + hz)
                E[r, 1, X + 1, own_y, :] = ey
                E[r, 2, X + 1, own_y, :] = E[r, 2, X + 1, own_y, :] + k * (xhi[s, r, 1] - hy)
                s_corner[b, r] = ey[Y - 1 : Y]

        @pl.when(sends_corner(s))
        def _():
            for r in reals:
                corner_copy(s, r).start()

    def update_h(r, planes):
        above = pl.ds(PAD + 1, Y)
        for p in planes:
            ex, ey, ez = (E[r, c, p, own_y, :] for c in range(3))
            curl_x = (E[r, 2, p, above, :] - ez) - (next_z(ey) - ey)
            curl_y = (next_z(ex) - ex) - (E[r, 2, p + 1, own_y, :] - ez)
            curl_z = (E[r, 1, p + 1, own_y, :] - ey) - (E[r, 0, p, above, :] - ex)
            for c, curl in enumerate((curl_x, curl_y, curl_z)):
                H[r, c, p, own_y, :] = H[r, c, p, own_y, :] - time_step * curl

    def update_e(r, planes):
        below = pl.ds(PAD - 1, Y)
        for p in planes:
            hx, hy, hz = (H[r, c, p, own_y, :] for c in range(3))
            curl_x = (hz - H[r, 2, p, below, :]) - (hy - last_z(hy))
            curl_y = (hx - last_z(hx)) - (hz - H[r, 2, p - 1, own_y, :])
            curl_z = (hy - H[r, 1, p - 1, own_y, :]) - (hx - H[r, 0, p, below, :])
            k = coef[r, p - 1]
            for c, curl in enumerate((curl_x, curl_y, curl_z)):
                E[r, c, p, own_y, :] = E[r, c, p, own_y, :] + k * (curl - J[c, p - 1])

    inner_h = range(1, X)
    inner_e = range(2, X)

    loads[1].wait()
    loads[2].wait()

    send_first()
    send_narrow(0)

    for load in loads[3:]:
        load.wait()

    receive_narrow(0)
    for r in reals:
        update_h(r, inner_h)

    if L > 1:
        for k in range(2):
            all_bytes(line.at[pl.ds(0, L - 1), pl.ds(0, packed)], k).wait()
    for there, k in ((has_left, 2), (has_right, 3)):

        @pl.when(there)
        def _():
            all_bytes(line.at[:, pl.ds(packed, half)], k).wait()

    for c in range(P_):
        a, b = jnp.int32(0), jnp.int32(0)
        for l in range(L):
            slab = slabs[l * P_ + j]
            a = jnp.where(slab == g * P_ + c, l, a)
            b = jnp.where(slab == g * P_ + c + 1, l, b)
        chosen[c, pl.ds(0, packed), :] = line[a, pl.ds(0, packed), :]
        chosen[c, pl.ds(packed, HY), :] = line[b, pl.ds(0, HY), :]
        chosen[c, pl.ds(packed + HY, half), :] = line[a, pl.ds(packed, half), :]
        chosen[c, pl.ds(packed + HY + half, 1), :] = line[b, pl.ds(packed, 1), :]
    found[j] = chosen[j]
    for d in range(1, P_):
        tile_copy(
            chosen.at[lax.rem(j + d, P_)], found.at[j], 2, in_plane(d), n
        ).start()

    mask_copy = pltpu.make_async_remote_copy(
        src_ref=mask.at[0],
        dst_ref=mask_up,
        send_sem=tile_sems.at[6],
        recv_sem=tile_sems.at[7],
        device_id=(w - 1, n),
        device_id_type=MESH,
    )

    if STEPS > 1:
        send_source(1)

    pl.when(has_down)(mask_copy.start)

    finish_up(0)
    finish_narrow(0)

    receive_corner(0)
    for r in reals:
        update_h(r, (X,))
    receive_up(0)

    if P_ > 1:
        for k in range(4, 6):
            all_bytes(found.at[pl.ds(0, P_ - 1)], k).wait()

    mine, following = jnp.int32(0), jnp.int32(0)
    for t in range(W):
        mine = jnp.where(slabs[t] == w, t % P_, mine)
        following = jnp.where(slabs[t] == w + 1, t % P_, following)
    total = found.shape[1]
    row = lax.broadcasted_iota(jnp.int32, (total, Z), 0)
    of_mine = (row < packed) | ((row >= packed + HY) & (row < packed + HY + half))
    block = jnp.where(of_mine, found[mine], found[following])
    refined = [
        exact_dot(block, refine_weights(2 * HZ, Z, 0, HZ - 1)),
        exact_dot(block, refine_weights(2 * HZ, Z, HZ, HZ - 1)),
    ]
    fine = lax.broadcasted_iota(jnp.int32, (Y, total), 0)
    source = lax.broadcasted_iota(jnp.int32, (Y, total), 1)
    cell = fine >> 1
    odd = (fine & 1) == 1

    def along_y(base, right):
        right = jnp.where(has_right, right, base + HY - 1)
        here = jnp.where(source == base + cell, jnp.where(odd, 0.5, 1.0), 0.0)
        next_cell = jnp.where(cell == HY - 1, right, base + cell + 1)
        return here + jnp.where(odd & (source == next_cell), 0.5, 0.0)

    weights = [along_y(p * HY, packed + HY + p) for p in range(half)]
    for p in range(TR):
        density[p] = exact_dot(weights[p % half], refined[p // half])
    beyond_last = exact_dot(along_y(packed, packed + HY + half), refined[0])
    density[TR] = jnp.where(has_up, beyond_last, density[TR - 1])

    level0, level1 = levels[0], levels[1]
    global_y = n * Y + lax.broadcasted_iota(jnp.int32, (Y, Z), 0)
    global_z = lax.broadcasted_iota(jnp.int32, (Y, Z), 1)
    inside_yz = (
        (global_y >= box[2]) & (global_y < box[3]) & (global_z >= box[4]) & (global_z < box[5])
    )

    def coefficients(value, x, background):
        global_x = w * X + x
        x_inside = (global_x >= box[0]) & (global_x < box[1])
        inside = inside_yz & jnp.broadcast_to(x_inside, (Y, Z))
        for r, threshold in enumerate(thresholds):
            low_end = math.tanh(sharpness * threshold)
            scale = low_end + math.tanh(sharpness * (1.0 - threshold))
            numer = low_end + jnp.tanh(sharpness * (value - threshold))
            design = level0 + (numer / scale) * (level1 - level0)
            coef[r, x] = time_step / jnp.where(inside, design, background)

    def own_coefficients(value, x):
        coefficients(value, x, jnp.where(mask[x] == 1, level1, level0))

    own_coefficients(0.5 * (density[TR - 1] + density[TR]), X - 1)

    def update_top(s):
        if s > 0:
            receive_corner(s)
            for r in reals:
                update_h(r, (X,))
        for r in reals:
            update_e(r, (X,))
        if s < STEPS - 1:
            send_up(s + 1)
            for r in reals:
                start_up(s + 1, r)

    update_top(0)

    own_coefficients(density[0], 0)
    for c in range(TR - 1):
        own_coefficients(0.5 * (density[c] + density[c + 1]), 2 * c + 1)
        own_coefficients(density[c + 1], 2 * c + 2)
    for r in reals:
        update_e(r, range(1, X))
    if STEPS > 1:
        send_narrow(1)

    @pl.when(has_up)
    def _():
        mask_copy.wait_recv()
        coefficients(density[TR], X, jnp.where(mask_up[...] == 1, level1, level0))

    pl.when(has_down)(mask_copy.wait_send)

    for s in range(1, STEPS):
        finish_source(s)
        receive_narrow(s)
        for r in reals:
            update_h(r, (1,))
        if s < STEPS - 1:
            send_source(s + 1)
        for r in reals:
            update_h(r, range(2, X))
        for r in reals:
            update_e(r, inner_e)
        finish_corner(s - 1)
        receive_source(s)
        finish_up(s)
        finish_narrow(s)
        if s == 1 and STEPS > 2:
            update_top(s)
        receive_up(s)
        if s == 1 and STEPS > 2:
            for r in reals:
                update_e(r, (1,))
        else:
            receive_corner(s)
            for r in reals:
                update_h(r, (X,))
            for r in reals:
                update_e(r, (1, X))
            if s < STEPS - 1:
                send_up(s + 1)
                for r in reals:
                    start_up(s + 1, r)
        if s < STEPS - 1:
            send_narrow(s + 1)

    finish_corner(STEPS - 1)


def write_out(e, h, e_out, h_out, sems):
    X, Y = e_out.shape[2:4]
    own = (slice(None), slice(None), pl.ds(1, X), pl.ds(PAD, Y), slice(None))
    copies = [
        pltpu.make_async_copy(e.at[own], e_out, sems.at[0]),
        pltpu.make_async_copy(h.at[own], h_out, sems.at[1]),
    ]
    for copy in copies:
        copy.start()
    for copy in copies:
        copy.wait()


def body(
    electric,
    magnetic,
    current,
    density_tiles,
    tile_slabs,
    design_box,
    material_mask,
    material_levels,
):
    W = lax.axis_size("wide")
    N = lax.axis_size("narrow")
    R, _, X, Y, Z = electric.shape
    TR, HY, HZ = density_tiles.shape
    f32 = jnp.float32
    hbm = pl.BlockSpec(memory_space=pl.ANY)
    vmem = pl.BlockSpec(memory_space=pltpu.VMEM)
    P_ = plane_size(W)
    L = W // P_
    half = TR // 2
    packed = half * HY
    total = -(-(packed + HY + half + 1) // 8) * 8
    dma = pltpu.SemaphoreType.DMA
    scratch = [
        pltpu.SMEM(tile_slabs.shape, jnp.int32),
        pltpu.SMEM(design_box.shape, jnp.int32),
        pltpu.SMEM(material_levels.shape, f32),
        pltpu.VMEM((3, X, Y, Z), f32),
        pltpu.VMEM((HY, TR, HZ), f32),
        pltpu.VMEM((X, Y, Z), jnp.int32),
        pltpu.VMEM((R, X + 1, Y, Z), f32),
        pltpu.VMEM((L, -(-(packed + half) // 8) * 8, Z), f32),
        pltpu.VMEM((P_, total, Z), f32),
        pltpu.VMEM((P_, total, Z), f32),
        pltpu.VMEM((TR + 1, Y, Z), f32),
        pltpu.VMEM((8, Z), f32),
        pltpu.VMEM((2, R, 2 * Y + 8, Z), f32),
        pltpu.VMEM((2, R, 2, Y, Z), f32),
        pltpu.VMEM((Y, Z), jnp.int32),
        pltpu.VMEM((STEPS, R, 2 * Y + 8, Z), f32),
        pltpu.VMEM((STEPS, R, 2, Y, Z), f32),
        pltpu.VMEM((2, R, 5, X, Z), f32),
        pltpu.VMEM((2, R, 5, X, Z), f32),
        pltpu.VMEM((2, R, 2, X, Z), f32),
        pltpu.VMEM((2, R, 2, X, Z), f32),
        pltpu.VMEM((2, R, 1, Z), f32),
        pltpu.VMEM((2, R, 1, Z), f32),
        pltpu.VMEM((R, 2, X, Z), f32),
        dma((8,)),
        dma((7,)),
        dma((STEPS, R)),
        dma((STEPS, R)),
        dma((2, R)),
        dma((2, R, 2)),
        dma((8,)),
    ]
    state = pltpu.VMEM((R, 3, X + 2, Y + 2 * PAD, Z), f32)
    e, h = pl.pallas_call(
        functools.partial(kernel, W, N),
        out_shape=(state, state),
        in_specs=[hbm] * 8,
        out_specs=(vmem,) * 2,
        scratch_shapes=scratch,
        compiler_params=pltpu.CompilerParams(
            collective_id=0, has_side_effects=True, vmem_limit_bytes=56623104
        ),
        name="window",
    )(
        tile_slabs,
        design_box,
        material_levels,
        electric,
        magnetic,
        current,
        jnp.transpose(density_tiles, (1, 0, 2)),
        material_mask,
    )
    out = jax.ShapeDtypeStruct(electric.shape, f32)
    return pl.pallas_call(
        write_out,
        out_shape=(out, out),
        in_specs=[vmem] * 2,
        out_specs=(hbm,) * 2,
        scratch_shapes=[dma((2,))],
        compiler_params=pltpu.CompilerParams(vmem_limit_bytes=2**20),
        name="write_out",
    )(e, h)


def solution(mesh):
    strip = P(None, None, "wide", "narrow", None)
    return jax.shard_map(
        body,
        mesh=mesh,
        in_specs=(
            strip,
            strip,
            P(None, "wide", "narrow", None),
            P("wide", "narrow", None),
            P(),
            P(),
            P("wide", "narrow", None),
            P(),
        ),
        out_specs=(strip, strip),
        check_vma=False,
    )
```
